256 devices in a mesh: tm: 8 (over z), sub: 32 (over y, x, core).
Axes of the slice: x: 4, y: 4, z: 8, core: 2. Of those that a mesh axis runs over, the one named last changes fastest.
Arguments:
- starts: float32 [8, 32, 16, 1024], P('tm', 'sub'), may hold values from -6 to 6
- inverses: float32 [32, 1024, 1024], P('sub')
- retain: float32 [32, 1024], P('sub'), may hold values from 0.4 to 1.1
- sources: float32 [32, 16, 1024], P('sub'), may hold values from -4 to 4
- coarse_decay: float32 [32, 1024], P('sub'), may hold values from 0.88 to 0.995
- admittance: float32 [32, 8], P('sub'), may hold values from 0.2 to 0.6
- partner: int32 [32, 8], P('sub'), may hold values from 0 to 255, as said below
- line_delay: int32 [32, 8], P('sub'), may hold values from 2 to 5, as said below
- line_live: int32 [32, 8], P('sub'), may hold values from 0 to 1, as said below
- term_block: int32 [32, 8], P('sub'), may hold values from 0 to 127, as said below
Outputs:
- ends: float32 [8, 32, 16, 1024], P('tm', 'sub')
The draws below stay inside these ranges and needn't reach their ends.
Inputs may be any that keep to these rules, and one draw needn't show every extreme that they name: Slots are paired: partner[i] = k exactly when partner[k] = i. A slot may be its own partner; such a slot is out of service. Of the slots of one index d of sub (its 1 subnetworks), exactly 1 are their own partners, and the others have partners on exactly 7 other indices, 1 slots on each and none elsewhere; these indices are d + 16 and pairs d + s and d - s modulo the number of indices. `line_delay`: paired slots have equal delays. `line_live`: paired slots are both in service or both not. `term_block`: the slots of one subnetwork have distinct blocks.
All inputs are finite; a program needn't handle non-finite values.
Results may differ from the reference program's by a relative error of at most 0.0001.
Values sent between devices are 32-bit elements; how exact they have to be, the bound alone decides.
A program may use at most 64 MiB of HBM per device.

```python
import math
import jax
import jax.numpy as jnp
from jax import lax

NODES = 1024
TERM = 8
LINES = 8
DMIN = 2
DMAX = 5
FINE = 4
SUB_DEV = 1
COLS = 16
SLICES = 8
SUBNETS = 32
NBLK = 128


def pairing(key):
    slots_dev = SUB_DEV * LINES
    devices_sub = SUBNETS // SUB_DEV
    half_way = devices_sub // 2
    capacity = max(1, 2 * slots_dev // devices_sub)
    groups = slots_dev // capacity
    paired_count = (groups - 2) // 2
    others = 2 + jax.random.permutation(jax.random.fold_in(key, 10), half_way - 2)[:paired_count - 1]
    shift_set = jnp.concatenate([jnp.ones((1,), jnp.int32), others.astype(jnp.int32)])
    perm_keys = jax.random.split(jax.random.fold_in(key, 11), devices_sub)
    placement = jax.vmap(lambda single: jax.random.permutation(single, slots_dev))(perm_keys).astype(jnp.int32)
    canonical = jnp.argsort(placement, axis=1).astype(jnp.int32)
    device_ids = jnp.arange(devices_sub, dtype=jnp.int32)[:, None]
    group_of = canonical // capacity
    paired_group = jnp.maximum(group_of - 2, 0)
    forward = paired_group % 2 == 0
    shift_each = shift_set[jnp.minimum(paired_group // 2, paired_count - 1)]
    pm_dev = jnp.where(forward, (device_ids + shift_each) % devices_sub, (device_ids - shift_each) % devices_sub)
    pm_canon = jnp.where(forward, canonical + capacity, canonical - capacity)
    peer_dev = jnp.where(group_of == 0, (device_ids + half_way) % devices_sub, jnp.where(group_of == 1, device_ids, pm_dev))
    peer_canon = jnp.where(group_of <= 1, canonical, pm_canon)
    mate = peer_dev * slots_dev + placement[peer_dev, peer_canon]
    mate = mate.reshape(-1).astype(jnp.int32)
    group_flat = group_of.reshape(-1)
    slots_all = SUBNETS * LINES
    own = jnp.arange(slots_all, dtype=jnp.int32)
    pair_key = jnp.minimum(own, mate)
    delays = jax.random.randint(jax.random.fold_in(key, 12), (slots_all,), DMIN, DMAX + 1).astype(jnp.int32)
    second = jnp.where(mate[0] == 1, 2, 1).astype(jnp.int32)
    second_key = jnp.minimum(second, mate[second])
    delays = delays.at[0].set(DMAX)
    delays = delays.at[second_key].set(DMIN)
    service = (jax.random.randint(jax.random.fold_in(key, 13), (slots_all,), 0, 4) > 0).astype(jnp.int32)
    service = service[pair_key]
    forced = (group_flat == 0) | (group_flat == 2) | (group_flat == 3)
    service = jnp.where(group_flat == 1, 0, jnp.where(forced, 1, service)).astype(jnp.int32)
    return (mate, delays[pair_key], service)


def draw_partner(key, part):
    return pairing(key)[0].reshape(SUBNETS, LINES).astype(jnp.int32)


def draw_line_delay(key, part):
    return pairing(key)[1].reshape(SUBNETS, LINES).astype(jnp.int32)


def draw_line_live(key, part):
    return pairing(key)[2].reshape(SUBNETS, LINES).astype(jnp.int32)


def draw_term_block(key, part):
    keys = jax.random.split(jax.random.fold_in(key, 14), SUBNETS)
    chosen = jax.vmap(lambda single: jax.random.permutation(single, NBLK)[:LINES])(keys)
    return chosen.astype(jnp.int32)


def draw_inverses(key, part):
    diagonal = 0.45 + 0.2 * jax.random.uniform(jax.random.fold_in(key, 21), (SUBNETS, NODES), jnp.float32)
    spread = jax.random.normal(jax.random.fold_in(key, 22), (SUBNETS, NODES, NODES), jnp.float32)
    spread = spread * (0.3 / NODES ** 0.5)
    return spread + diagonal[:, :, None] * jnp.eye(NODES, dtype=jnp.float32)[None]


def levels(stream_key, extent, cuts, low, high):
    gain, own = 1.0, jax.random.fold_in(stream_key, 6)
    for axis_at, shards_of in cuts:
        heights = jnp.exp(jax.random.uniform(jax.random.fold_in(own, axis_at), (shards_of,), jnp.float32, low / len(cuts), high / len(cuts)))
        gain = gain * jnp.repeat(heights, extent[axis_at] // shards_of).reshape([-1 if axis == axis_at else 1 for axis in range(len(extent))])
    return gain


def normal_values(own_key, extent, width, limit, shards=(), held_as=jnp.bfloat16):
    factor_of = levels(own_key, extent, shards, -0.22, 0.18) if shards else 1.0
    array = jax.random.normal(own_key, extent, jnp.float32) * width * factor_of
    return jnp.minimum(jnp.maximum(array, -limit), limit).astype(held_as)


def setup_inputs(seed: int = 0) -> dict:
    key_list = jax.random.split(jax.random.key(seed), 11)
    return {
        "starts": normal_values(key_list[0], (SLICES, SUBNETS, COLS, NODES), 1.0, 6.0, ((0, 8), (1, 32)), jnp.float32),
        "inverses": draw_inverses(jax.random.fold_in(key_list[10], 71), 0),
        "retain": jnp.clip(jnp.exp(math.log(1.1) - 1.011601 * jax.random.uniform(key_list[2], (SUBNETS, NODES), jnp.float32) ** levels(key_list[2], (SUBNETS, NODES), ((0, 32),), -0.2, 0.2)), 0.4, 1.1),
        "sources": normal_values(key_list[3], (SUBNETS, COLS, NODES), 0.5, 4.0, ((0, 32),), jnp.float32),
        "coarse_decay": jnp.clip(jnp.exp(math.log(0.995) - 0.12282084 * jax.random.uniform(key_list[4], (SUBNETS, NODES), jnp.float32) ** levels(key_list[4], (SUBNETS, NODES), ((0, 32),), -0.2, 0.2)), 0.88, 0.995),
        "admittance": jnp.clip(jnp.exp(math.log(0.6) - 1.0986123 * jax.random.uniform(key_list[5], (SUBNETS, LINES), jnp.float32) ** levels(key_list[5], (SUBNETS, LINES), ((0, 32),), -0.2, 0.2)), 0.2, 0.6),
        "partner": draw_partner(jax.random.fold_in(key_list[10], 71), 0),
        "line_delay": draw_line_delay(jax.random.fold_in(key_list[10], 71), 0),
        "line_live": draw_line_live(jax.random.fold_in(key_list[10], 71), 0),
        "term_block": draw_term_block(jax.random.fold_in(key_list[10], 71), 0),
    }


def terminals(state, term_block):
    grouped = state.reshape(state.shape[0], state.shape[1], state.shape[2], state.shape[3] // TERM, TERM)
    target = (state.shape[0], state.shape[1], state.shape[2], term_block.shape[1], TERM)
    picked = jnp.take_along_axis(grouped, jnp.broadcast_to(term_block[None, :, None, :, None], target), axis=3)
    picked = jnp.transpose(picked, (1, 3, 0, 2, 4))
    return picked.reshape(picked.shape[0] * picked.shape[1], picked.shape[2], picked.shape[3] * TERM)


def inject(collected, partner, line_delay, line_live, admittance, term_block, step, state):
    reach = jnp.maximum(step + 1 - line_delay, 0).reshape(-1).astype(jnp.int32)
    stacked = jnp.concatenate(collected, axis=0)
    everyone = collected[0].shape[0]
    row_index = (reach * everyone + partner.reshape(-1)).astype(jnp.int32)
    far_values = stacked[row_index]
    far_values = far_values.reshape(term_block.shape[0], term_block.shape[1], state.shape[0], state.shape[2], TERM)
    weights = admittance * line_live.astype(jnp.float32)
    far_values = far_values * weights[:, :, None, None, None]
    blocks_here = jnp.arange(state.shape[3] // TERM, dtype=jnp.int32)
    onehot = (term_block[:, :, None] == blocks_here[None, None, :]).astype(jnp.float32)
    placed = jnp.einsum('plsct,plb->spcbt', far_values, onehot, precision=lax.Precision.HIGHEST)
    return placed.reshape(state.shape)


def advance(state, inverses, retain, sources, injected):
    driven = retain[None, :, None, :] * state + sources[None] + injected
    return jnp.einsum('spcm,pnm->spcn', driven, inverses, precision=lax.Precision.HIGHEST, preferred_element_type=jnp.float32)


def reference(starts, inverses, retain, sources, coarse_decay, admittance, partner, line_delay, line_live, term_block):
    state = starts
    collected = [terminals(state, term_block)]
    for step in range(FINE):
        injected = inject(collected, partner, line_delay, line_live, admittance, term_block, step, state)
        state = advance(state, inverses, retain, sources, injected)
        if step + 1 <= FINE - DMIN:
            collected.append(terminals(state, term_block))
    offsets = state - coarse_decay[None, :, None, :] * starts
    current = starts[0]
    finals = []
    for slice_index in range(SLICES):
        current = coarse_decay[:, None, :] * current + offsets[slice_index]
        finals.append(current)
    return jnp.stack(finals)
```

```python
import functools

import jax
import jax.numpy as jnp
from jax import lax
from jax.experimental import pallas as pl
from jax.experimental.pallas import tpu as pltpu
from jax.sharding import PartitionSpec as P

TERM = 8
LINES = 8
COLS = 16
LANES = 128
NODES = 1024
CHUNKS = 8
MESH = pl.DeviceIdType.MESH
F32 = jnp.float32
BF16 = jnp.bfloat16


def split(x):
    high = x.astype(BF16)
    low = (x - high.astype(F32)).astype(BF16)
    return high, low


def dot(a, b):
    return jnp.dot(a, b, preferred_element_type=F32)


def packed(ref, at, offset):
    group = lax.broadcasted_iota(jnp.int32, (LINES, LANES), 1) // COLS
    out = jnp.zeros((LINES, LANES), F32)
    for t in range(TERM):
        rows = ref[at, pl.ds(t, LINES, stride=TERM), :]
        shift = (COLS * t - offset) % LANES
        rows = pltpu.roll(rows, shift, 1) if shift else rows
        out = jnp.where(group == t, rows, out)
    return out


def unpacked(far):
    return jnp.concatenate(
        [far] + [pltpu.roll(far, LANES - COLS * t, 1) for t in range(1, TERM)], axis=0
    )


def kernel(
    slices, subs,
    starts_h, inverses_h, retain_h, sources_h, decay_h,
    admittance, partner, delay, live, block,
    out_ref,
    starts, sources, retain, decay,
    raw, a_high, a_low, z_all, z_turned, z_both, m_high, m_low,
    rows, near0, near12, ends_in, far0, far1,
    in_sems, raw_sems, send_sems, recv0, recv12, z_send, z_recv,
):
    zed = lax.axis_index("tm")
    me = lax.axis_index("sub")

    far0[...] = jnp.zeros_like(far0)
    far1[...] = jnp.zeros_like(far1)

    barrier = pltpu.get_barrier_semaphore()

    @pl.loop(1, subs)
    def _(o):
        pl.semaphore_signal(
            barrier, inc=1, device_id={"sub": lax.rem(me + o, subs)}, device_id_type=MESH
        )

    @pl.loop(1, slices)
    def _(o):
        pl.semaphore_signal(
            barrier, inc=1, device_id={"tm": lax.rem(zed + o, slices)}, device_id_type=MESH
        )

    pairs = (
        (starts_h, starts), (retain_h, retain), (sources_h, sources), (decay_h, decay),
    )
    loads = [pltpu.make_async_copy(a, b, in_sems.at[k]) for k, (a, b) in enumerate(pairs)]
    depth = NODES // CHUNKS
    chunks = [
        pltpu.make_async_copy(
            inverses_h.at[pl.ds(k * depth, depth), :], raw.at[pl.ds(k * depth, depth), :],
            raw_sems.at[k],
        )
        for k in range(CHUNKS)
    ]
    for load in loads:
        load.start()
    for chunk in chunks:
        chunk.start()
    for load in loads:
        load.wait()

    gain = retain[...]
    inverse_gain = 1.0 / gain
    lane = lax.broadcasted_iota(jnp.int32, (LINES, NODES), 1)
    slot = lax.broadcasted_iota(jnp.int32, (LINES, NODES), 0)
    first = jnp.zeros((LINES, NODES), jnp.int32)
    for l in range(LINES):
        first = jnp.where(slot == l, block[0, l] * TERM, first)
    ones = [(lane == first + t).astype(F32) for t in range(TERM)]
    inputs = jnp.concatenate(
        [
            starts[...],
            sources[...] * inverse_gain,
            jnp.zeros((COLS, NODES), F32),
            jnp.broadcast_to(inverse_gain, (COLS, NODES)),
        ]
        + ones,
        axis=0,
    )
    turned = jnp.transpose(inputs)
    z_all[0] = turned.reshape(NODES // TERM, TERM, LANES)

    def pick(at):
        for l in range(LINES):
            rows[at, pl.ds(l * TERM, TERM), :] = z_all[at, block[0, l]]

    pick(0)
    near0[me] = packed(rows, 0, 0)

    pl.semaphore_wait(barrier, subs - 1 + slices - 1)

    def sub_copy(ref, send, recv, o):
        return pltpu.make_async_remote_copy(
            src_ref=ref.at[me], dst_ref=ref.at[me], send_sem=send, recv_sem=recv,
            device_id={"sub": lax.rem(me + o, subs)}, device_id_type=MESH,
        )

    def all_of(ref, send, recv):
        whole = ref.at[pl.ds(0, subs - 1)]
        return pltpu.make_async_remote_copy(
            src_ref=whole, dst_ref=whole, send_sem=send, recv_sem=recv,
            device_id={"sub": lax.rem(me + 1, subs)}, device_id_type=MESH,
        )

    @pl.loop(1, subs)
    def _(o):
        sub_copy(near0, send_sems.at[0], recv0, o).start()

    slot8 = lax.broadcasted_iota(jnp.int32, (LINES, LANES), 0)
    weight = jnp.zeros((LINES, LANES), F32)
    for l in range(LINES):
        weight = jnp.where(slot8 == l, admittance[0, l] * live[0, l].astype(F32), weight)
    weight = weight * packed(rows, 0, 3 * COLS)

    high, low = split(turned)
    z_both[:, :LANES] = high
    z_both[:, LANES:] = low
    for k in range(CHUNKS):
        chunks[k].wait()
        piece = pl.ds(k * depth, depth)
        high, low = split(raw[piece, :] * gain)
        a_high[piece, :] = high
        a_low[piece, :] = low

    @pl.loop(1, 5)
    def _(k):
        both = z_both[...]
        y = dot(a_high[...], both) + dot(a_low[...], both)
        new = y[:, :LANES] + y[:, LANES:]
        z_all[k] = new.reshape(NODES // TERM, TERM, LANES)
        high, low = split(new)
        z_both[:, :LANES] = high
        z_both[:, LANES:] = low
        z_turned[k - 1] = jnp.transpose(new)

    mine_z = pl.ds(pl.multiple_of(zed * COLS, COLS), COLS)
    base = z_turned[3, :COLS, :]
    for k in range(4):
        base = base + z_turned[k, COLS : 2 * COLS, :]
    slope = decay[...]
    base = jnp.where(zed == 0, base, base - slope * starts[...])
    ends_in[mine_z, :] = base

    def z_copy(ref, which, d):
        return pltpu.make_async_remote_copy(
            src_ref=ref.at[mine_z, :], dst_ref=ref.at[mine_z, :],
            send_sem=z_send.at[which, d], recv_sem=z_recv.at[which, d],
            device_id={"tm": lax.rem(zed + d, slices)}, device_id_type=MESH,
        )

    def z_start(ref, which):
        @pl.loop(1, slices)
        def _(d):
            @pl.when(zed + d < slices)
            def _():
                z_copy(ref, which, d).start()

    def z_arrive(ref, which):
        @pl.loop(1, slices)
        def _(d):
            @pl.when(zed >= d)
            def _():
                z_copy(ref, which, d).wait_recv()

    def z_sent(ref, which):
        @pl.loop(1, slices)
        def _(d):
            @pl.when(zed + d < slices)
            def _():
                z_copy(ref, which, d).wait_send()

    z_start(ends_in, 0)

    pick(1)
    pick(2)
    lanes64 = lax.broadcasted_iota(jnp.int32, (LINES * TERM, LANES), 1)
    first_rows = rows[1]
    second_rows = rows[2] + jnp.where(lanes64 >= COLS, first_rows, 0.0)
    q_high, q_low = split(jnp.concatenate([first_rows, second_rows], axis=0))
    q_both = jnp.concatenate([q_high, q_low], axis=1)
    r32 = lax.broadcasted_iota(jnp.int32, (4 * COLS, LANES), 0)
    c32 = lax.broadcasted_iota(jnp.int32, (4 * COLS, LANES), 1)
    unit = jnp.where(
        (c32 < COLS) & (r32 < 2 * COLS) & ((r32 == c32) | (r32 == c32 + COLS)), 1.0, 0.0
    ).astype(F32)

    all_of(near0, send_sems.at[0], recv0).wait_recv()
    def row_of(tile, l):
        return jnp.sum(jnp.where(slot8 == lax.rem(partner[0, l], LINES), tile, 0.0), axis=0, keepdims=True)

    olds = jnp.zeros((LINES, LANES), F32)
    for l in range(LINES):
        olds = jnp.where(slot8 == l, row_of(near0[lax.div(partner[0, l], LINES)], l), olds)
    spread0 = unpacked(olds * weight)
    e_high, e_low = split(jnp.concatenate([unit, spread0], axis=0))
    e_both = jnp.concatenate([e_high, e_low], axis=1)
    e_both = jnp.concatenate([e_both, e_both], axis=0)
    s = dot(q_both, e_both)
    s = s[:, :LANES] + s[:, LANES:]
    rows[1] = s[: LINES * TERM]
    rows[2] = s[LINES * TERM :]
    near12[me, 0] = packed(rows, 1, 0)
    near12[me, 1] = packed(rows, 2, 0)

    @pl.loop(1, subs)
    def _(o):
        sub_copy(near12, send_sems.at[1], recv12, o).start()

    blank = jnp.zeros((LINES * TERM, LANES), F32)
    far0[mine_z, :] = jnp.transpose(jnp.concatenate([spread0, blank], axis=0))[:COLS]
    z_start(far0, 1)

    half = LINES * TERM
    effect = jnp.concatenate(
        [
            z_turned[2, half:, :] + z_turned[3, half:, :],
            jnp.zeros((half, NODES), F32),
            z_turned[1, half:, :],
            z_turned[0, half:, :],
        ],
        axis=0,
    )
    high, low = split(effect)
    m_high[...] = high
    m_low[...] = low

    all_of(near12, send_sems.at[1], recv12).wait_recv()
    fars = []
    for step in (2, 3):
        far = olds
        for l in range(LINES):
            reach = step + 1 - delay[0, l]
            late = jnp.minimum(jnp.maximum(reach, 1), 2) - 1
            row = row_of(near12[lax.div(partner[0, l], LINES), late], l)
            far = jnp.where((slot8 == l) & (jnp.full((LINES, LANES), reach, jnp.int32) > 0), row, far)
        fars.append(unpacked(far * weight))
    spread = jnp.concatenate(fars, axis=0)
    far1[mine_z, :] = jnp.transpose(spread)[:COLS]
    z_start(far1, 2)

    z_arrive(ends_in, 0)

    def one(i, state):
        return slope * state + ends_in[pl.ds(pl.multiple_of(i * COLS, COLS), COLS), :]

    plain = lax.fori_loop(0, zed + 1, one, jnp.zeros((COLS, NODES), F32))

    z_arrive(far0, 1)
    z_arrive(far1, 2)
    high, low = split(jnp.concatenate([far0[...], far1[...]], axis=1))
    count = slices * COLS
    y = dot(jnp.concatenate([high, low], axis=0), m_high[...])
    y = y[:count] + y[count:] + dot(high, m_low[...])
    state = jnp.zeros((COLS, NODES), F32)
    for i in range(slices):
        state = jnp.where(i <= zed, slope * state + y[i * COLS : (i + 1) * COLS], state)
    out_ref[...] = plain + state

    all_of(near0, send_sems.at[0], recv0).wait_send()
    all_of(near12, send_sems.at[1], recv12).wait_send()
    z_sent(ends_in, 0)
    z_sent(far0, 1)
    z_sent(far1, 2)


def shards(slices, subs, starts, inverses, retain, sources, decay, admittance, partner, delay, live, block):
    vmem, smem = pltpu.VMEM, pltpu.SMEM
    out = pl.pallas_call(
        functools.partial(kernel, slices, subs),
        out_shape=jax.ShapeDtypeStruct((COLS, NODES), F32),
        in_specs=[pl.BlockSpec(memory_space=pltpu.HBM)] * 5 + [pl.BlockSpec(memory_space=smem)] * 5,
        out_specs=pl.BlockSpec(memory_space=pltpu.VMEM),
        scratch_shapes=[
            vmem((COLS, NODES), F32), vmem((COLS, NODES), F32),
            vmem((1, NODES), F32), vmem((1, NODES), F32),
            vmem((NODES, NODES), F32), vmem((NODES, NODES), BF16), vmem((NODES, NODES), BF16),
            vmem((5, NODES // TERM, TERM, LANES), F32), vmem((4, LANES, NODES), F32),
            vmem((NODES, 2 * LANES), BF16),
            vmem((2 * LANES, NODES), BF16), vmem((2 * LANES, NODES), BF16),
            vmem((3, LINES * TERM, LANES), F32),
            vmem((subs, LINES, LANES), F32), vmem((subs, 2, LINES, LANES), F32),
            vmem((slices * COLS, NODES), F32),
            vmem((slices * COLS, LANES), F32), vmem((slices * COLS, LANES), F32),
            pltpu.SemaphoreType.DMA((4,)), pltpu.SemaphoreType.DMA((CHUNKS,)),
            pltpu.SemaphoreType.DMA((2,)), pltpu.SemaphoreType.DMA, pltpu.SemaphoreType.DMA,
            pltpu.SemaphoreType.DMA((3, slices)), pltpu.SemaphoreType.DMA((3, slices)),
        ],
        compiler_params=pltpu.CompilerParams(
            collective_id=0, has_side_effects=True, vmem_limit_bytes=48 * 1024 * 1024
        ),
    )(
        starts.reshape(COLS, NODES), inverses.reshape(NODES, NODES), retain,
        sources.reshape(COLS, NODES), decay, admittance, partner, delay, live, block,
    )
    return out.reshape(1, 1, COLS, NODES)


def solution(mesh):
    return jax.shard_map(
        functools.partial(shards, mesh.shape["tm"], mesh.shape["sub"]),
        mesh=mesh,
        in_specs=(
            P("tm", "sub", None, None),
            P("sub", None, None),
            P("sub", None),
            P("sub", None, None),
            P("sub", None),
            P("sub", None),
            P("sub", None),
            P("sub", None),
            P("sub", None),
            P("sub", None),
        ),
        out_specs=P("tm", "sub", None, None),
        check_vma=False,
    )
```

```python
import functools

import jax
import jax.numpy as jnp
from jax import lax
from jax.experimental import pallas as pl
from jax.experimental.pallas import tpu as pltpu
from jax.sharding import PartitionSpec as P

TERM = 8
LINES = 8
COLS = 16
LANES = 128
NODES = 1024
CHUNKS = 8
MESH = pl.DeviceIdType.MESH
F32 = jnp.float32
BF16 = jnp.bfloat16


def split(x):
    high = x.astype(BF16)
    low = (x - high.astype(F32)).astype(BF16)
    return high, low


def dot(a, b):
    return jnp.dot(a, b, preferred_element_type=F32)


def packed(ref, at, offset):
    group = lax.broadcasted_iota(jnp.int32, (LINES, LANES), 1) // COLS
    out = jnp.zeros((LINES, LANES), F32)
    for t in range(TERM):
        rows = ref[at, pl.ds(t, LINES, stride=TERM), :]
        shift = (COLS * t - offset) % LANES
        rows = pltpu.roll(rows, shift, 1) if shift else rows
        out = jnp.where(group == t, rows, out)
    return out


def unpacked(far):
    return jnp.concatenate(
        [far] + [pltpu.roll(far, LANES - COLS * t, 1) for t in range(1, TERM)], axis=0
    )


def kernel(
    slices, subs,
    starts_h, inverses_h, retain_h, sources_h, decay_h,
    admittance_h, partner_h, delay_h, live_h, block_h,
    out_ref,
    starts, sources, retain, decay, admittance, partner, delay, live, block,
    raw, a_high, a_low, z_all, z_turned, z_both, m_high, m_low,
    rows, near0, near12, ends_in, far0, far1,
    in_sems, raw_sems, send_sems, recv0, recv12, z_send, z_recv,
):
    zed = lax.axis_index("tm")
    me = lax.axis_index("sub")

    far0[...] = jnp.zeros_like(far0)
    far1[...] = jnp.zeros_like(far1)

    barrier = pltpu.get_barrier_semaphore()

    @pl.loop(1, subs)
    def _(o):
        pl.semaphore_signal(
            barrier, inc=1, device_id={"sub": lax.rem(me + o, subs)}, device_id_type=MESH
        )

    @pl.loop(1, slices)
    def _(o):
        pl.semaphore_signal(
            barrier, inc=1, device_id={"tm": lax.rem(zed + o, slices)}, device_id_type=MESH
        )

    pairs = (
        (starts_h, starts), (block_h, block), (retain_h, retain), (sources_h, sources),
        (partner_h, partner), (admittance_h, admittance), (live_h, live), (delay_h, delay),
        (decay_h, decay),
    )
    loads = [pltpu.make_async_copy(a, b, in_sems.at[k]) for k, (a, b) in enumerate(pairs)]
    depth = NODES // CHUNKS
    chunks = [
        pltpu.make_async_copy(
            inverses_h.at[pl.ds(k * depth, depth), :], raw.at[pl.ds(k * depth, depth), :],
            raw_sems.at[k],
        )
        for k in range(CHUNKS)
    ]
    for load in loads:
        load.start()
    for chunk in chunks:
        chunk.start()
    for load in loads:
        load.wait()

    gain = retain[...]
    inverse_gain = 1.0 / gain
    lane = lax.broadcasted_iota(jnp.int32, (LINES, NODES), 1)
    slot = lax.broadcasted_iota(jnp.int32, (LINES, NODES), 0)
    first = jnp.zeros((LINES, NODES), jnp.int32)
    for l in range(LINES):
        first = jnp.where(slot == l, block[0, l] * TERM, first)
    ones = [(lane == first + t).astype(F32) for t in range(TERM)]
    inputs = jnp.concatenate(
        [
            starts[...],
            sources[...] * inverse_gain,
            jnp.zeros((COLS, NODES), F32),
            jnp.broadcast_to(inverse_gain, (COLS, NODES)),
        ]
        + ones,
        axis=0,
    )
    turned = jnp.transpose(inputs)
    z_all[0] = turned.reshape(NODES // TERM, TERM, LANES)

    def pick(at):
        for l in range(LINES):
            rows[at, pl.ds(l * TERM, TERM), :] = z_all[at, block[0, l]]

    pick(0)
    near0[me] = packed(rows, 0, 0)

    pl.semaphore_wait(barrier, subs - 1 + slices - 1)

    def sub_copy(ref, send, recv, o):
        return pltpu.make_async_remote_copy(
            src_ref=ref.at[me], dst_ref=ref.at[me], send_sem=send, recv_sem=recv,
            device_id={"sub": lax.rem(me + o, subs)}, device_id_type=MESH,
        )

    def all_of(ref, send, recv):
        whole = ref.at[pl.ds(0, subs - 1)]
        return pltpu.make_async_remote_copy(
            src_ref=whole, dst_ref=whole, send_sem=send, recv_sem=recv,
            device_id={"sub": lax.rem(me + 1, subs)}, device_id_type=MESH,
        )

    @pl.loop(1, subs)
    def _(o):
        sub_copy(near0, send_sems.at[0], recv0, o).start()

    slot8 = lax.broadcasted_iota(jnp.int32, (LINES, LANES), 0)
    weight = jnp.zeros((LINES, LANES), F32)
    for l in range(LINES):
        weight = jnp.where(slot8 == l, admittance[0, l] * live[0, l].astype(F32), weight)
    weight = weight * packed(rows, 0, 3 * COLS)

    high, low = split(turned)
    z_both[:, :LANES] = high
    z_both[:, LANES:] = low
    for k in range(CHUNKS):
        chunks[k].wait()
        piece = pl.ds(k * depth, depth)
        high, low = split(raw[piece, :] * gain)
        a_high[piece, :] = high
        a_low[piece, :] = low

    @pl.loop(1, 5)
    def _(k):
        both = z_both[...]
        y = dot(a_high[...], both) + dot(a_low[...], both)
        new = y[:, :LANES] + y[:, LANES:]
        z_all[k] = new.reshape(NODES // TERM, TERM, LANES)
        high, low = split(new)
        z_both[:, :LANES] = high
        z_both[:, LANES:] = low
        z_turned[k - 1] = jnp.transpose(new)

    mine_z = pl.ds(pl.multiple_of(zed * COLS, COLS), COLS)
    base = z_turned[3, :COLS, :]
    for k in range(4):
        base = base + z_turned[k, COLS : 2 * COLS, :]
    slope = decay[...]
    base = jnp.where(zed == 0, base, base - slope * starts[...])
    ends_in[mine_z, :] = base

    def z_copy(ref, which, d):
        return pltpu.make_async_remote_copy(
            src_ref=ref.at[mine_z, :], dst_ref=ref.at[mine_z, :],
            send_sem=z_send.at[which, d], recv_sem=z_recv.at[which, d],
            device_id={"tm": lax.rem(zed + d, slices)}, device_id_type=MESH,
        )

    def z_start(ref, which):
        @pl.loop(1, slices)
        def _(d):
            @pl.when(zed + d < slices)
            def _():
                z_copy(ref, which, d).start()

    def z_arrive(ref, which):
        @pl.loop(1, slices)
        def _(d):
            @pl.when(zed >= d)
            def _():
                z_copy(ref, which, d).wait_recv()

    def z_sent(ref, which):
        @pl.loop(1, slices)
        def _(d):
            @pl.when(zed + d < slices)
            def _():
                z_copy(ref, which, d).wait_send()

    z_start(ends_in, 0)

    pick(1)
    pick(2)
    lanes64 = lax.broadcasted_iota(jnp.int32, (LINES * TERM, LANES), 1)
    first_rows = rows[1]
    second_rows = rows[2] + jnp.where(lanes64 >= COLS, first_rows, 0.0)
    q_high, q_low = split(jnp.concatenate([first_rows, second_rows], axis=0))
    q_both = jnp.concatenate([q_high, q_low], axis=1)
    r32 = lax.broadcasted_iota(jnp.int32, (4 * COLS, LANES), 0)
    c32 = lax.broadcasted_iota(jnp.int32, (4 * COLS, LANES), 1)
    unit = jnp.where(
        (c32 < COLS) & (r32 < 2 * COLS) & ((r32 == c32) | (r32 == c32 + COLS)), 1.0, 0.0
    ).astype(F32)

    all_of(near0, send_sems.at[0], recv0).wait_recv()
    def row_of(tile, l):
        return jnp.sum(jnp.where(slot8 == lax.rem(partner[0, l], LINES), tile, 0.0), axis=0, keepdims=True)

    olds = jnp.zeros((LINES, LANES), F32)
    for l in range(LINES):
        olds = jnp.where(slot8 == l, row_of(near0[lax.div(partner[0, l], LINES)], l), olds)
    spread0 = unpacked(olds * weight)
    e_high, e_low = split(jnp.concatenate([unit, spread0], axis=0))
    e_both = jnp.concatenate([e_high, e_low], axis=1)
    e_both = jnp.concatenate([e_both, e_both], axis=0)
    s = dot(q_both, e_both)
    s = s[:, :LANES] + s[:, LANES:]
    rows[1] = s[: LINES * TERM]
    rows[2] = s[LINES * TERM :]
    near12[me, 0] = packed(rows, 1, 0)
    near12[me, 1] = packed(rows, 2, 0)

    @pl.loop(1, subs)
    def _(o):
        sub_copy(near12, send_sems.at[1], recv12, o).start()

    blank = jnp.zeros((LINES * TERM, LANES), F32)
    far0[mine_z, :] = jnp.transpose(jnp.concatenate([spread0, blank], axis=0))[:COLS]
    z_start(far0, 1)

    half = LINES * TERM
    effect = jnp.concatenate(
        [
            z_turned[2, half:, :] + z_turned[3, half:, :],
            jnp.zeros((half, NODES), F32),
            z_turned[1, half:, :],
            z_turned[0, half:, :],
        ],
        axis=0,
    )
    high, low = split(effect)
    m_high[...] = high
    m_low[...] = low

    all_of(near12, send_sems.at[1], recv12).wait_recv()
    fars = []
    for step in (2, 3):
        far = olds
        for l in range(LINES):
            reach = step + 1 - delay[0, l]
            late = jnp.minimum(jnp.maximum(reach, 1), 2) - 1
            row = row_of(near12[lax.div(partner[0, l], LINES), late], l)
            far = jnp.where((slot8 == l) & (jnp.full((LINES, LANES), reach, jnp.int32) > 0), row, far)
        fars.append(unpacked(far * weight))
    spread = jnp.concatenate(fars, axis=0)
    far1[mine_z, :] = jnp.transpose(spread)[:COLS]
    z_start(far1, 2)

    z_arrive(ends_in, 0)

    def one(i, state):
        return slope * state + ends_in[pl.ds(pl.multiple_of(i * COLS, COLS), COLS), :]

    plain = lax.fori_loop(0, zed + 1, one, jnp.zeros((COLS, NODES), F32))

    z_arrive(far0, 1)
    z_arrive(far1, 2)
    high, low = split(jnp.concatenate([far0[...], far1[...]], axis=1))
    count = slices * COLS
    y = dot(jnp.concatenate([high, low], axis=0), m_high[...])
    y = y[:count] + y[count:] + dot(high, m_low[...])
    state = jnp.zeros((COLS, NODES), F32)
    for i in range(slices):
        state = jnp.where(i <= zed, slope * state + y[i * COLS : (i + 1) * COLS], state)
    out_ref[...] = plain + state

    all_of(near0, send_sems.at[0], recv0).wait_send()
    all_of(near12, send_sems.at[1], recv12).wait_send()
    z_sent(ends_in, 0)
    z_sent(far0, 1)
    z_sent(far1, 2)


def shards(slices, subs, starts, inverses, retain, sources, decay, admittance, partner, delay, live, block):
    vmem, smem = pltpu.VMEM, pltpu.SMEM
    out = pl.pallas_call(
        functools.partial(kernel, slices, subs),
        out_shape=jax.ShapeDtypeStruct((COLS, NODES), F32),
        in_specs=[pl.BlockSpec(memory_space=pltpu.HBM)] * 10,
        out_specs=pl.BlockSpec(memory_space=pltpu.VMEM),
        scratch_shapes=[
            vmem((COLS, NODES), F32), vmem((COLS, NODES), F32),
            vmem((1, NODES), F32), vmem((1, NODES), F32),
            smem((1, LINES), F32), smem((1, LINES), jnp.int32), smem((1, LINES), jnp.int32),
            smem((1, LINES), jnp.int32), smem((1, LINES), jnp.int32),
            vmem((NODES, NODES), F32), vmem((NODES, NODES), BF16), vmem((NODES, NODES), BF16),
            vmem((5, NODES // TERM, TERM, LANES), F32), vmem((4, LANES, NODES), F32),
            vmem((NODES, 2 * LANES), BF16),
            vmem((2 * LANES, NODES), BF16), vmem((2 * LANES, NODES), BF16),
            vmem((3, LINES * TERM, LANES), F32),
            vmem((subs, LINES, LANES), F32), vmem((subs, 2, LINES, LANES), F32),
            vmem((slices * COLS, NODES), F32),
            vmem((slices * COLS, LANES), F32), vmem((slices * COLS, LANES), F32),
            pltpu.SemaphoreType.DMA((9,)), pltpu.SemaphoreType.DMA((CHUNKS,)),
            pltpu.SemaphoreType.DMA((2,)), pltpu.SemaphoreType.DMA, pltpu.SemaphoreType.DMA,
            pltpu.SemaphoreType.DMA((3, slices)), pltpu.SemaphoreType.DMA((3, slices)),
        ],
        compiler_params=pltpu.CompilerParams(
            collective_id=0, has_side_effects=True, vmem_limit_bytes=67043328
        ),
    )(
        starts.reshape(COLS, NODES), inverses.reshape(NODES, NODES), retain,
        sources.reshape(COLS, NODES), decay, admittance, partner, delay, live, block,
    )
    return out.reshape(1, 1, COLS, NODES)


def solution(mesh):
    return jax.shard_map(
        functools.partial(shards, mesh.shape["tm"], mesh.shape["sub"]),
        mesh=mesh,
        in_specs=(
            P("tm", "sub", None, None),
            P("sub", None, None),
            P("sub", None),
            P("sub", None, None),
            P("sub", None),
            P("sub", None),
            P("sub", None),
            P("sub", None),
            P("sub", None),
            P("sub", None),
        ),
        out_specs=P("tm", "sub", None, None),
        check_vma=False,
    )
```

```python
import functools

import jax
import jax.numpy as jnp
from jax import lax
from jax.experimental import pallas as pl
from jax.experimental.pallas import tpu as pltpu
from jax.sharding import PartitionSpec as P

TERM = 8
LINES = 8
COLS = 16
LANES = 128
NODES = 1024
CHUNKS = 8
MESH = pl.DeviceIdType.MESH
F32 = jnp.float32
BF16 = jnp.bfloat16


def split(x):
    high = x.astype(BF16)
    low = (x - high.astype(F32)).astype(BF16)
    return high, low


def dot(a, b):
    return jnp.dot(a, b, preferred_element_type=F32)


def packed(ref, at, offset):
    group = lax.broadcasted_iota(jnp.int32, (LINES, LANES), 1) // COLS
    out = jnp.zeros((LINES, LANES), F32)
    for t in range(TERM):
        rows = ref[at, pl.ds(t, LINES, stride=TERM), :]
        shift = (COLS * t - offset) % LANES
        rows = pltpu.roll(rows, shift, 1) if shift else rows
        out = jnp.where(group == t, rows, out)
    return out


def unpacked(far):
    return jnp.concatenate(
        [far] + [pltpu.roll(far, LANES - COLS * t, 1) for t in range(1, TERM)], axis=0
    )


def kernel(
    slices, subs,
    starts_h, inverses_h, retain_h, sources_h, decay_h,
    admittance_h, partner_h, delay_h, live_h, block_h,
    out_ref,
    starts, sources, retain, decay, admittance, partner, delay, live, block,
    raw, a_high, a_low, z_all, z_turned, z_both, m_high, m_low,
    rows, near0, near12, offset, parts_in, sums, plain, far0, far1,
    in_sems, raw_sems, send_sems, recv0, recv12, z_send, z_recv,
    part_send, part_recv, sum_send, sum_recv, ready,
):
    group = slices // 2
    zed = lax.axis_index("tm")
    me = lax.axis_index("sub")

    far0[...] = jnp.zeros_like(far0)
    far1[...] = jnp.zeros_like(far1)

    barrier = pltpu.get_barrier_semaphore()

    @pl.loop(1, subs)
    def _(o):
        pl.semaphore_signal(
            barrier, inc=1, device_id={"sub": lax.rem(me + o, subs)}, device_id_type=MESH
        )

    @pl.loop(1, slices)
    def _(o):
        @pl.when(zed + o < slices)
        def _():
            pl.semaphore_signal(
                barrier, inc=1, device_id={"tm": lax.rem(zed + o, slices)}, device_id_type=MESH
            )

    pairs = (
        (starts_h, starts), (block_h, block), (retain_h, retain), (sources_h, sources),
        (partner_h, partner), (admittance_h, admittance), (live_h, live), (delay_h, delay),
        (decay_h, decay),
    )
    loads = [pltpu.make_async_copy(a, b, in_sems.at[k]) for k, (a, b) in enumerate(pairs)]
    depth = NODES // CHUNKS
    chunks = [
        pltpu.make_async_copy(
            inverses_h.at[pl.ds(k * depth, depth), :], raw.at[pl.ds(k * depth, depth), :],
            raw_sems.at[k],
        )
        for k in range(CHUNKS)
    ]
    for load in loads:
        load.start()
    for chunk in chunks:
        chunk.start()
    for load in loads:
        load.wait()

    gain = retain[...]
    inverse_gain = 1.0 / gain
    lane = lax.broadcasted_iota(jnp.int32, (LINES, NODES), 1)
    slot = lax.broadcasted_iota(jnp.int32, (LINES, NODES), 0)
    first = jnp.zeros((LINES, NODES), jnp.int32)
    for l in range(LINES):
        first = jnp.where(slot == l, block[0, l] * TERM, first)
    ones = [(lane == first + t).astype(F32) for t in range(TERM)]
    inputs = jnp.concatenate(
        [
            starts[...],
            sources[...] * inverse_gain,
            jnp.zeros((COLS, NODES), F32),
            jnp.broadcast_to(inverse_gain, (COLS, NODES)),
        ]
        + ones,
        axis=0,
    )
    turned = jnp.transpose(inputs)
    z_all[0] = turned.reshape(NODES // TERM, TERM, LANES)

    def pick(at):
        for l in range(LINES):
            rows[at, pl.ds(l * TERM, TERM), :] = z_all[at, block[0, l]]

    pick(0)
    near0[me] = packed(rows, 0, 0)

    pl.semaphore_wait(barrier, subs - 1 + zed)

    @pl.loop(1, slices)
    def _(o):
        @pl.when(zed >= o)
        def _():
            pl.semaphore_signal(
                ready, inc=1, device_id={"tm": lax.rem(zed + slices - o, slices)},
                device_id_type=MESH,
            )

    def sub_copy(ref, send, recv, o):
        return pltpu.make_async_remote_copy(
            src_ref=ref.at[me], dst_ref=ref.at[me], send_sem=send, recv_sem=recv,
            device_id={"sub": lax.rem(me + o, subs)}, device_id_type=MESH,
        )

    def all_of(ref, send, recv):
        whole = ref.at[pl.ds(0, subs - 1)]
        return pltpu.make_async_remote_copy(
            src_ref=whole, dst_ref=whole, send_sem=send, recv_sem=recv,
            device_id={"sub": lax.rem(me + 1, subs)}, device_id_type=MESH,
        )

    @pl.loop(1, subs)
    def _(o):
        sub_copy(near0, send_sems.at[0], recv0, o).start()

    slot8 = lax.broadcasted_iota(jnp.int32, (LINES, LANES), 0)
    weight = jnp.zeros((LINES, LANES), F32)
    for l in range(LINES):
        weight = jnp.where(slot8 == l, admittance[0, l] * live[0, l].astype(F32), weight)
    weight = weight * packed(rows, 0, 3 * COLS)

    high, low = split(turned)
    z_both[:, :LANES] = high
    z_both[:, LANES:] = low
    for k in range(CHUNKS):
        chunks[k].wait()
        piece = pl.ds(k * depth, depth)
        high, low = split(raw[piece, :] * gain)
        a_high[piece, :] = high
        a_low[piece, :] = low

    @pl.loop(1, 5)
    def _(k):
        both = z_both[...]
        y = dot(a_high[...], both) + dot(a_low[...], both)
        new = y[:, :LANES] + y[:, LANES:]
        z_all[k] = new.reshape(NODES // TERM, TERM, LANES)
        high, low = split(new)
        z_both[:, :LANES] = high
        z_both[:, LANES:] = low
        z_turned[k - 1] = jnp.transpose(new)

    mine_z = pl.ds(pl.multiple_of(zed * COLS, COLS), COLS)
    base = z_turned[3, :COLS, :]
    for k in range(4):
        base = base + z_turned[k, COLS : 2 * COLS, :]
    slope = decay[...]
    base = jnp.where(zed == 0, base, base - slope * starts[...])
    width = NODES // group
    for k in range(group):
        offset[k] = base[:, k * width : (k + 1) * width]
    side = lax.div(zed, group)
    place = lax.rem(zed, group)
    parts_in[zed] = offset[place]

    def part_copy(to, sender):
        return pltpu.make_async_remote_copy(
            src_ref=offset.at[lax.rem(to, group)], dst_ref=parts_in.at[zed],
            send_sem=part_send.at[to], recv_sem=part_recv.at[sender],
            device_id={"tm": to}, device_id_type=MESH,
        )

    def sum_copy(to, owner):
        return pltpu.make_async_remote_copy(
            src_ref=sums.at[to], dst_ref=plain.at[place],
            send_sem=sum_send.at[to], recv_sem=sum_recv.at[owner],
            device_id={"tm": side * group + to}, device_id_type=MESH,
        )

    @pl.when(zed < slices - 1)
    def _():
        pl.semaphore_wait(ready, slices - 1 - zed)

    @pl.loop(0, slices)
    def _(to):
        @pl.when((lax.div(to, group) >= side) & (to != zed))
        def _():
            part_copy(to, zed).start()

    def z_copy(ref, which, d):
        return pltpu.make_async_remote_copy(
            src_ref=ref.at[mine_z, :], dst_ref=ref.at[mine_z, :],
            send_sem=z_send.at[which, d], recv_sem=z_recv.at[which, d],
            device_id={"tm": lax.rem(zed + d, slices)}, device_id_type=MESH,
        )

    def z_start(ref, which):
        @pl.loop(1, slices)
        def _(d):
            @pl.when(zed + d < slices)
            def _():
                z_copy(ref, which, d).start()

    def z_arrive(ref, which):
        @pl.loop(1, slices)
        def _(d):
            @pl.when(zed >= d)
            def _():
                z_copy(ref, which, d).wait_recv()

    def z_sent(ref, which):
        @pl.loop(1, slices)
        def _(d):
            @pl.when(zed + d < slices)
            def _():
                z_copy(ref, which, d).wait_send()

    pick(1)
    pick(2)
    lanes64 = lax.broadcasted_iota(jnp.int32, (LINES * TERM, LANES), 1)
    first_rows = rows[1]
    second_rows = rows[2] + jnp.where(lanes64 >= COLS, first_rows, 0.0)
    q_high, q_low = split(jnp.concatenate([first_rows, second_rows], axis=0))
    q_both = jnp.concatenate([q_high, q_low], axis=1)
    r32 = lax.broadcasted_iota(jnp.int32, (4 * COLS, LANES), 0)
    c32 = lax.broadcasted_iota(jnp.int32, (4 * COLS, LANES), 1)
    unit = jnp.where(
        (c32 < COLS) & (r32 < 2 * COLS) & ((r32 == c32) | (r32 == c32 + COLS)), 1.0, 0.0
    ).astype(F32)

    all_of(near0, send_sems.at[0], recv0).wait_recv()
    def row_of(tile, l):
        return jnp.sum(jnp.where(slot8 == lax.rem(partner[0, l], LINES), tile, 0.0), axis=0, keepdims=True)

    olds = jnp.zeros((LINES, LANES), F32)
    for l in range(LINES):
        olds = jnp.where(slot8 == l, row_of(near0[lax.div(partner[0, l], LINES)], l), olds)
    spread0 = unpacked(olds * weight)
    e_high, e_low = split(jnp.concatenate([unit, spread0], axis=0))
    e_both = jnp.concatenate([e_high, e_low], axis=1)
    e_both = jnp.concatenate([e_both, e_both], axis=0)
    s = dot(q_both, e_both)
    s = s[:, :LANES] + s[:, LANES:]
    rows[1] = s[: LINES * TERM]
    rows[2] = s[LINES * TERM :]
    near12[me, 0] = packed(rows, 1, 0)
    near12[me, 1] = packed(rows, 2, 0)

    @pl.loop(1, subs)
    def _(o):
        sub_copy(near12, send_sems.at[1], recv12, o).start()

    blank = jnp.zeros((LINES * TERM, LANES), F32)
    far0[mine_z, :] = jnp.transpose(jnp.concatenate([spread0, blank], axis=0))[:COLS]
    z_start(far0, 0)

    half = LINES * TERM
    effect = jnp.concatenate(
        [
            z_turned[2, half:, :] + z_turned[3, half:, :],
            jnp.zeros((half, NODES), F32),
            z_turned[1, half:, :],
            z_turned[0, half:, :],
        ],
        axis=0,
    )
    high, low = split(effect)
    m_high[...] = high
    m_low[...] = low

    all_of(near12, send_sems.at[1], recv12).wait_recv()
    fars = []
    for step in (2, 3):
        far = olds
        for l in range(LINES):
            reach = step + 1 - delay[0, l]
            late = jnp.minimum(jnp.maximum(reach, 1), 2) - 1
            row = row_of(near12[lax.div(partner[0, l], LINES), late], l)
            far = jnp.where((slot8 == l) & (jnp.full((LINES, LANES), reach, jnp.int32) > 0), row, far)
        fars.append(unpacked(far * weight))
    spread = jnp.concatenate(fars, axis=0)
    far1[mine_z, :] = jnp.transpose(spread)[:COLS]
    z_start(far1, 1)

    @pl.loop(0, slices)
    def _(sender):
        @pl.when((lax.div(sender, group) <= side) & (sender != zed))
        def _():
            part_copy(zed, sender).wait_recv()

    bend = decay[:, pl.ds(pl.multiple_of(place * width, LANES), width)]

    def one(i, state):
        return bend * state + parts_in[i]

    state = lax.fori_loop(0, side * group, one, jnp.zeros((COLS, width), F32))
    for k in range(group):
        state = bend * state + parts_in[side * group + k]
        sums[k] = state
    plain[place] = sums[place]

    @pl.loop(0, group)
    def _(to):
        @pl.when(to != place)
        def _():
            sum_copy(to, place).start()

    @pl.loop(0, group)
    def _(owner):
        @pl.when(owner != place)
        def _():
            sum_copy(owner, owner).wait_recv()

    z_arrive(far0, 0)
    z_arrive(far1, 1)
    high, low = split(jnp.concatenate([far0[...], far1[...]], axis=1))
    count = slices * COLS
    y = dot(jnp.concatenate([high, low], axis=0), m_high[...])
    y = y[:count] + y[count:] + dot(high, m_low[...])
    state = jnp.zeros((COLS, NODES), F32)
    for i in range(slices):
        state = jnp.where(i <= zed, slope * state + y[i * COLS : (i + 1) * COLS], state)
    for k in range(group):
        part = slice(k * width, (k + 1) * width)
        out_ref[:, part] = plain[k] + state[:, part]

    all_of(near0, send_sems.at[0], recv0).wait_send()
    all_of(near12, send_sems.at[1], recv12).wait_send()

    @pl.loop(0, slices)
    def _(to):
        @pl.when((lax.div(to, group) >= side) & (to != zed))
        def _():
            part_copy(to, zed).wait_send()

    @pl.loop(0, group)
    def _(to):
        @pl.when(to != place)
        def _():
            sum_copy(to, place).wait_send()

    z_sent(far0, 0)
    z_sent(far1, 1)


def shards(slices, subs, starts, inverses, retain, sources, decay, admittance, partner, delay, live, block):
    vmem, smem = pltpu.VMEM, pltpu.SMEM
    group = slices // 2
    out = pl.pallas_call(
        functools.partial(kernel, slices, subs),
        out_shape=jax.ShapeDtypeStruct((COLS, NODES), F32),
        in_specs=[pl.BlockSpec(memory_space=pltpu.HBM)] * 10,
        out_specs=pl.BlockSpec(memory_space=pltpu.VMEM),
        scratch_shapes=[
            vmem((COLS, NODES), F32), vmem((COLS, NODES), F32),
            vmem((1, NODES), F32), vmem((1, NODES), F32),
            smem((1, LINES), F32), smem((1, LINES), jnp.int32), smem((1, LINES), jnp.int32),
            smem((1, LINES), jnp.int32), smem((1, LINES), jnp.int32),
            vmem((NODES, NODES), F32), vmem((NODES, NODES), BF16), vmem((NODES, NODES), BF16),
            vmem((5, NODES // TERM, TERM, LANES), F32), vmem((4, LANES, NODES), F32),
            vmem((NODES, 2 * LANES), BF16),
            vmem((2 * LANES, NODES), BF16), vmem((2 * LANES, NODES), BF16),
            vmem((3, LINES * TERM, LANES), F32),
            vmem((subs, LINES, LANES), F32), vmem((subs, 2, LINES, LANES), F32),
            vmem((group, COLS, NODES // group), F32), vmem((slices, COLS, NODES // group), F32),
            vmem((group, COLS, NODES // group), F32), vmem((group, COLS, NODES // group), F32),
            vmem((slices * COLS, LANES), F32), vmem((slices * COLS, LANES), F32),
            pltpu.SemaphoreType.DMA((9,)), pltpu.SemaphoreType.DMA((CHUNKS,)),
            pltpu.SemaphoreType.DMA((2,)), pltpu.SemaphoreType.DMA, pltpu.SemaphoreType.DMA,
            pltpu.SemaphoreType.DMA((2, slices)), pltpu.SemaphoreType.DMA((2, slices)),
            pltpu.SemaphoreType.DMA((slices,)), pltpu.SemaphoreType.DMA((slices,)),
            pltpu.SemaphoreType.DMA((group,)), pltpu.SemaphoreType.DMA((group,)),
            pltpu.SemaphoreType.REGULAR,
        ],
        compiler_params=pltpu.CompilerParams(
            collective_id=0, has_side_effects=True, vmem_limit_bytes=67043328
        ),
    )(
        starts.reshape(COLS, NODES), inverses.reshape(NODES, NODES), retain,
        sources.reshape(COLS, NODES), decay, admittance, partner, delay, live, block,
    )
    return out.reshape(1, 1, COLS, NODES)


def solution(mesh):
    return jax.shard_map(
        functools.partial(shards, mesh.shape["tm"], mesh.shape["sub"]),
        mesh=mesh,
        in_specs=(
            P("tm", "sub", None, None),
            P("sub", None, None),
            P("sub", None),
            P("sub", None, None),
            P("sub", None),
            P("sub", None),
            P("sub", None),
            P("sub", None),
            P("sub", None),
            P("sub", None),
        ),
        out_specs=P("tm", "sub", None, None),
        check_vma=False,
    )
```

```python
import functools

import jax
import jax.numpy as jnp
from jax import lax
from jax.experimental import pallas as pl
from jax.experimental.pallas import tpu as pltpu
from jax.sharding import PartitionSpec as P

TERM = 8
LINES = 8
COLS = 16
LANES = 128
NODES = 1024
CHUNKS = 8
MESH = pl.DeviceIdType.MESH
F32 = jnp.float32
BF16 = jnp.bfloat16


def split(x):
    high = x.astype(BF16)
    low = (x - high.astype(F32)).astype(BF16)
    return high, low


def dot(a, b):
    return jnp.dot(a, b, preferred_element_type=F32)


def packed(ref, at, offset):
    group = lax.broadcasted_iota(jnp.int32, (LINES, LANES), 1) // COLS
    out = jnp.zeros((LINES, LANES), F32)
    for t in range(TERM):
        rows = ref[at, pl.ds(t, LINES, stride=TERM), :]
        shift = (COLS * t - offset) % LANES
        rows = pltpu.roll(rows, shift, 1) if shift else rows
        out = jnp.where(group == t, rows, out)
    return out


def unpacked(far):
    return jnp.concatenate(
        [far] + [pltpu.roll(far, LANES - COLS * t, 1) for t in range(1, TERM)], axis=0
    )


def kernel(
    slices, subs,
    starts_h, inverses_h, retain_h, sources_h, decay_h,
    admittance_h, partner_h, delay_h, live_h, block_h,
    out_ref,
    starts, sources, retain, decay, admittance, partner, delay, live, block,
    raw, a_high, a_low, z_all, z_turned, z_both, m_high, m_low,
    rows, near0, near12, offset, parts_in, half_in, prefix, far0, far1,
    in_sems, raw_sems, send_sems, recv0, recv12, z_send, z_recv,
    part_send, part_recv, half_send, half_recv, prefix_send, prefix_recv, ready,
):
    group = slices // 2
    zed = lax.axis_index("tm")
    me = lax.axis_index("sub")

    far0[...] = jnp.zeros_like(far0)
    far1[...] = jnp.zeros_like(far1)
    prefix[...] = jnp.zeros_like(prefix)

    pairs = (
        (starts_h, starts), (block_h, block), (retain_h, retain), (sources_h, sources),
        (partner_h, partner), (admittance_h, admittance), (live_h, live), (delay_h, delay),
        (decay_h, decay),
    )
    loads = [pltpu.make_async_copy(a, b, in_sems.at[k]) for k, (a, b) in enumerate(pairs)]
    depth = NODES // CHUNKS
    chunks = [
        pltpu.make_async_copy(
            inverses_h.at[pl.ds(k * depth, depth), :], raw.at[pl.ds(k * depth, depth), :],
            raw_sems.at[k],
        )
        for k in range(CHUNKS)
    ]
    for load in loads:
        load.start()
    for chunk in chunks:
        chunk.start()
    barrier = pltpu.get_barrier_semaphore()

    @pl.loop(1, subs)
    def _(o):
        pl.semaphore_signal(
            barrier, inc=1, device_id={"sub": lax.rem(me + o, subs)}, device_id_type=MESH
        )

    @pl.loop(1, slices)
    def _(o):
        @pl.when(zed + o < slices)
        def _():
            pl.semaphore_signal(
                barrier, inc=1, device_id={"tm": lax.rem(zed + o, slices)}, device_id_type=MESH
            )

    for load in loads:
        load.wait()

    gain = retain[...]
    inverse_gain = 1.0 / gain
    lane = lax.broadcasted_iota(jnp.int32, (LINES, NODES), 1)
    slot = lax.broadcasted_iota(jnp.int32, (LINES, NODES), 0)
    first = jnp.zeros((LINES, NODES), jnp.int32)
    for l in range(LINES):
        first = jnp.where(slot == l, block[0, l] * TERM, first)
    ones = [(lane == first + t).astype(F32) for t in range(TERM)]
    inputs = jnp.concatenate(
        [
            starts[...],
            sources[...] * inverse_gain,
            jnp.zeros((COLS, NODES), F32),
            jnp.broadcast_to(inverse_gain, (COLS, NODES)),
        ]
        + ones,
        axis=0,
    )
    turned = jnp.transpose(inputs)
    z_all[0] = turned.reshape(NODES // TERM, TERM, LANES)

    def pick(at):
        for l in range(LINES):
            rows[at, pl.ds(l * TERM, TERM), :] = z_all[at, block[0, l]]

    pick(0)
    near0[me] = packed(rows, 0, 0)

    pl.semaphore_wait(barrier, subs - 1 + zed)

    @pl.loop(1, slices)
    def _(o):
        @pl.when(zed >= o)
        def _():
            pl.semaphore_signal(
                ready.at[zed], inc=1, device_id={"tm": lax.rem(zed + slices - o, slices)},
                device_id_type=MESH,
            )

    def sub_copy(ref, send, recv, o):
        return pltpu.make_async_remote_copy(
            src_ref=ref.at[me], dst_ref=ref.at[me], send_sem=send, recv_sem=recv,
            device_id={"sub": lax.rem(me + o, subs)}, device_id_type=MESH,
        )

    def all_of(ref, send, recv):
        whole = ref.at[pl.ds(0, subs - 1)]
        return pltpu.make_async_remote_copy(
            src_ref=whole, dst_ref=whole, send_sem=send, recv_sem=recv,
            device_id={"sub": lax.rem(me + 1, subs)}, device_id_type=MESH,
        )

    @pl.loop(1, subs)
    def _(o):
        sub_copy(near0, send_sems.at[0], recv0, o).start()

    slot8 = lax.broadcasted_iota(jnp.int32, (LINES, LANES), 0)
    weight = jnp.zeros((LINES, LANES), F32)
    for l in range(LINES):
        weight = jnp.where(slot8 == l, admittance[0, l] * live[0, l].astype(F32), weight)
    weight = weight * packed(rows, 0, 3 * COLS)

    high, low = split(turned)
    z_both[:, :LANES] = high
    z_both[:, LANES:] = low
    for k in range(CHUNKS):
        chunks[k].wait()
        piece = pl.ds(k * depth, depth)
        high, low = split(raw[piece, :] * gain)
        a_high[piece, :] = high
        a_low[piece, :] = low

    def advance(k):
        both = z_both[...]
        y = dot(a_high[...], both) + dot(a_low[...], both)
        new = y[:, :LANES] + y[:, LANES:]
        z_all[k] = new.reshape(NODES // TERM, TERM, LANES)
        high, low = split(new)
        z_both[:, :LANES] = high
        z_both[:, LANES:] = low
        z_turned[k - 1] = jnp.transpose(new)

    @pl.loop(1, 4)
    def _(k):
        advance(k)

    pick(1)
    pick(2)
    lanes64 = lax.broadcasted_iota(jnp.int32, (LINES * TERM, LANES), 1)
    first_rows = rows[1]
    second_rows = rows[2] + jnp.where(lanes64 >= COLS, first_rows, 0.0)
    q_high, q_low = split(jnp.concatenate([first_rows, second_rows], axis=0))
    q_both = jnp.concatenate([q_high, q_low], axis=1)
    r32 = lax.broadcasted_iota(jnp.int32, (4 * COLS, LANES), 0)
    c32 = lax.broadcasted_iota(jnp.int32, (4 * COLS, LANES), 1)
    unit = jnp.where(
        (c32 < COLS) & (r32 < 2 * COLS) & ((r32 == c32) | (r32 == c32 + COLS)), 1.0, 0.0
    ).astype(F32)

    all_of(near0, send_sems.at[0], recv0).wait_recv()
    def row_of(tile, l):
        return jnp.sum(jnp.where(slot8 == lax.rem(partner[0, l], LINES), tile, 0.0), axis=0, keepdims=True)

    olds = jnp.zeros((LINES, LANES), F32)
    for l in range(LINES):
        olds = jnp.where(slot8 == l, row_of(near0[lax.div(partner[0, l], LINES)], l), olds)
    spread0 = unpacked(olds * weight)
    e_high, e_low = split(jnp.concatenate([unit, spread0], axis=0))
    e_both = jnp.concatenate([e_high, e_low], axis=1)
    e_both = jnp.concatenate([e_both, e_both], axis=0)
    s = dot(q_both, e_both)
    s = s[:, :LANES] + s[:, LANES:]
    rows[1] = s[: LINES * TERM]
    rows[2] = s[LINES * TERM :]
    near12[me, 0] = packed(rows, 1, 0)
    near12[me, 1] = packed(rows, 2, 0)

    @pl.loop(1, subs)
    def _(o):
        sub_copy(near12, send_sems.at[1], recv12, o).start()

    advance(4)

    mine_z = pl.ds(pl.multiple_of(zed * COLS, COLS), COLS)
    base = z_turned[3, :COLS, :]
    for k in range(4):
        base = base + z_turned[k, COLS : 2 * COLS, :]
    slope = decay[...]
    base = jnp.where(zed == 0, base, base - slope * starts[...])
    width = NODES // group
    for k in range(group):
        offset[k] = base[:, k * width : (k + 1) * width]
    side = lax.div(zed, group)
    place = lax.rem(zed, group)
    half_in[place] = offset[...]

    def half_copy(to, sender):
        return pltpu.make_async_remote_copy(
            src_ref=offset, dst_ref=half_in.at[place],
            send_sem=half_send.at[to], recv_sem=half_recv.at[sender],
            device_id={"tm": side * group + to}, device_id_type=MESH,
        )

    def part_copy(to, sender):
        return pltpu.make_async_remote_copy(
            src_ref=offset.at[to], dst_ref=parts_in.at[place],
            send_sem=part_send.at[to], recv_sem=part_recv.at[sender],
            device_id={"tm": group + to}, device_id_type=MESH,
        )

    def prefix_copy(to, owner):
        return pltpu.make_async_remote_copy(
            src_ref=prefix.at[place], dst_ref=prefix.at[place],
            send_sem=prefix_send.at[to], recv_sem=prefix_recv.at[owner],
            device_id={"tm": group + to}, device_id_type=MESH,
        )

    @pl.loop(0, group)
    def _(to):
        @pl.when(to > place)
        def _():
            pl.semaphore_wait(ready.at[side * group + to], 1)
            half_copy(to, place).start()

    @pl.when(side == 0)
    def _():
        @pl.loop(0, group)
        def _(to):
            pl.semaphore_wait(ready.at[group + to], 1)
            part_copy(to, place).start()

    def z_copy(ref, which, d):
        return pltpu.make_async_remote_copy(
            src_ref=ref.at[mine_z, :], dst_ref=ref.at[mine_z, :],
            send_sem=z_send.at[which, d], recv_sem=z_recv.at[which, d],
            device_id={"tm": lax.rem(zed + d, slices)}, device_id_type=MESH,
        )

    def z_start(ref, which):
        @pl.loop(1, slices)
        def _(d):
            @pl.when(zed + d < slices)
            def _():
                z_copy(ref, which, d).start()

    def z_arrive(ref, which):
        @pl.loop(1, slices)
        def _(d):
            @pl.when(zed >= d)
            def _():
                z_copy(ref, which, d).wait_recv()

    def z_sent(ref, which):
        @pl.loop(1, slices)
        def _(d):
            @pl.when(zed + d < slices)
            def _():
                z_copy(ref, which, d).wait_send()

    blank = jnp.zeros((LINES * TERM, LANES), F32)
    far0[mine_z, :] = jnp.transpose(jnp.concatenate([spread0, blank], axis=0))[:COLS]
    z_start(far0, 0)

    half = LINES * TERM
    effect = jnp.concatenate(
        [
            z_turned[2, half:, :] + z_turned[3, half:, :],
            jnp.zeros((half, NODES), F32),
            z_turned[1, half:, :],
            z_turned[0, half:, :],
        ],
        axis=0,
    )
    high, low = split(effect)
    m_high[...] = high
    m_low[...] = low

    all_of(near12, send_sems.at[1], recv12).wait_recv()
    fars = []
    for step in (2, 3):
        far = olds
        for l in range(LINES):
            reach = step + 1 - delay[0, l]
            late = jnp.minimum(jnp.maximum(reach, 1), 2) - 1
            row = row_of(near12[lax.div(partner[0, l], LINES), late], l)
            far = jnp.where((slot8 == l) & (jnp.full((LINES, LANES), reach, jnp.int32) > 0), row, far)
        fars.append(unpacked(far * weight))
    spread = jnp.concatenate(fars, axis=0)
    far1[mine_z, :] = jnp.transpose(spread)[:COLS]
    z_start(far1, 1)

    @pl.when(side == 1)
    def _():
        @pl.loop(0, group)
        def _(sender):
            part_copy(sender, sender).wait_recv()

        bend = decay[:, pl.ds(pl.multiple_of(place * width, LANES), width)]
        state = parts_in[0]
        for k in range(1, group):
            state = bend * state + parts_in[k]
        prefix[place] = state

        @pl.loop(0, group)
        def _(to):
            @pl.when(to != place)
            def _():
                prefix_copy(to, place).start()

    @pl.loop(0, group)
    def _(sender):
        @pl.when(sender < place)
        def _():
            half_copy(sender, sender).wait_recv()

    @pl.when(side == 1)
    def _():
        @pl.loop(0, group)
        def _(owner):
            @pl.when(owner != place)
            def _():
                prefix_copy(owner, owner).wait_recv()

    bends = [slope[:, k * width : (k + 1) * width] for k in range(group)]

    def one(i, states):
        return tuple(bends[k] * states[k] + half_in[i, k] for k in range(group))

    plain = lax.fori_loop(0, place + 1, one, tuple(prefix[k] for k in range(group)))

    z_arrive(far0, 0)
    z_arrive(far1, 1)
    high, low = split(jnp.concatenate([far0[...], far1[...]], axis=1))
    count = slices * COLS
    y = dot(jnp.concatenate([high, low], axis=0), m_high[...])
    y = y[:count] + y[count:] + dot(high, m_low[...])
    state = jnp.zeros((COLS, NODES), F32)
    for i in range(slices):
        state = jnp.where(i <= zed, slope * state + y[i * COLS : (i + 1) * COLS], state)
    for k in range(group):
        part = slice(k * width, (k + 1) * width)
        out_ref[:, part] = plain[k] + state[:, part]

    all_of(near0, send_sems.at[0], recv0).wait_send()
    all_of(near12, send_sems.at[1], recv12).wait_send()

    @pl.loop(0, group)
    def _(to):
        @pl.when(to > place)
        def _():
            half_copy(to, place).wait_send()

    @pl.when(side == 0)
    def _():
        @pl.loop(0, group)
        def _(to):
            part_copy(to, place).wait_send()

    @pl.when(side == 1)
    def _():
        @pl.loop(0, group)
        def _(to):
            @pl.when(to != place)
            def _():
                prefix_copy(to, place).wait_send()

    z_sent(far0, 0)
    z_sent(far1, 1)


def shards(slices, subs, starts, inverses, retain, sources, decay, admittance, partner, delay, live, block):
    vmem, smem = pltpu.VMEM, pltpu.SMEM
    group = slices // 2
    out = pl.pallas_call(
        functools.partial(kernel, slices, subs),
        out_shape=jax.ShapeDtypeStruct((COLS, NODES), F32),
        in_specs=[pl.BlockSpec(memory_space=pltpu.HBM)] * 10,
        out_specs=pl.BlockSpec(memory_space=pltpu.VMEM),
        scratch_shapes=[
            vmem((COLS, NODES), F32), vmem((COLS, NODES), F32),
            vmem((1, NODES), F32), vmem((1, NODES), F32),
            smem((1, LINES), F32), smem((1, LINES), jnp.int32), smem((1, LINES), jnp.int32),
            smem((1, LINES), jnp.int32), smem((1, LINES), jnp.int32),
            vmem((NODES, NODES), F32), vmem((NODES, NODES), BF16), vmem((NODES, NODES), BF16),
            vmem((5, NODES // TERM, TERM, LANES), F32), vmem((4, LANES, NODES), F32),
            vmem((NODES, 2 * LANES), BF16),
            vmem((2 * LANES, NODES), BF16), vmem((2 * LANES, NODES), BF16),
            vmem((3, LINES * TERM, LANES), F32),
            vmem((subs, LINES, LANES), F32), vmem((subs, 2, LINES, LANES), F32),
            vmem((group, COLS, NODES // group), F32), vmem((group, COLS, NODES // group), F32),
            vmem((group, group, COLS, NODES // group), F32),
            vmem((group, COLS, NODES // group), F32),
            vmem((slices * COLS, LANES), F32), vmem((slices * COLS, LANES), F32),
            pltpu.SemaphoreType.DMA((9,)), pltpu.SemaphoreType.DMA((CHUNKS,)),
            pltpu.SemaphoreType.DMA((2,)), pltpu.SemaphoreType.DMA, pltpu.SemaphoreType.DMA,
            pltpu.SemaphoreType.DMA((2, slices)), pltpu.SemaphoreType.DMA((2, slices)),
            pltpu.SemaphoreType.DMA((group,)), pltpu.SemaphoreType.DMA((group,)),
            pltpu.SemaphoreType.DMA((group,)), pltpu.SemaphoreType.DMA((group,)),
            pltpu.SemaphoreType.DMA((group,)), pltpu.SemaphoreType.DMA((group,)),
            pltpu.SemaphoreType.REGULAR((slices,)),
        ],
        compiler_params=pltpu.CompilerParams(
            collective_id=0, has_side_effects=True, vmem_limit_bytes=67043328
        ),
    )(
        starts.reshape(COLS, NODES), inverses.reshape(NODES, NODES), retain,
        sources.reshape(COLS, NODES), decay, admittance, partner, delay, live, block,
    )
    return out.reshape(1, 1, COLS, NODES)


def solution(mesh):
    return jax.shard_map(
        functools.partial(shards, mesh.shape["tm"], mesh.shape["sub"]),
        mesh=mesh,
        in_specs=(
            P("tm", "sub", None, None),
            P("sub", None, None),
            P("sub", None),
            P("sub", None, None),
            P("sub", None),
            P("sub", None),
            P("sub", None),
            P("sub", None),
            P("sub", None),
            P("sub", None),
        ),
        out_specs=P("tm", "sub", None, None),
        check_vma=False,
    )
```

```python
import functools

import jax
import jax.numpy as jnp
from jax import lax
from jax.experimental import pallas as pl
from jax.experimental.pallas import tpu as pltpu
from jax.sharding import PartitionSpec as P

TERM = 8
LINES = 8
COLS = 16
LANES = 128
NODES = 1024
CHUNKS = 8
MESH = pl.DeviceIdType.MESH
F32 = jnp.float32
BF16 = jnp.bfloat16


def split(x):
    high = x.astype(BF16)
    low = (x - high.astype(F32)).astype(BF16)
    return high, low


def dot(a, b):
    return jnp.dot(a, b, preferred_element_type=F32)


def packed(ref, at, offset):
    group = lax.broadcasted_iota(jnp.int32, (LINES, LANES), 1) // COLS
    out = jnp.zeros((LINES, LANES), F32)
    for t in range(TERM):
        rows = ref[at, pl.ds(t, LINES, stride=TERM), :]
        shift = (COLS * t - offset) % LANES
        rows = pltpu.roll(rows, shift, 1) if shift else rows
        out = jnp.where(group == t, rows, out)
    return out


def unpacked(far):
    return jnp.concatenate(
        [far] + [pltpu.roll(far, LANES - COLS * t, 1) for t in range(1, TERM)], axis=0
    )


def kernel(
    slices, subs,
    starts_h, inverses_h, retain_h, sources_h, decay_h,
    admittance_h, partner_h, delay_h, live_h, block_h,
    out_ref,
    starts, sources, retain, decay, admittance, partner, delay, live, block,
    raw, a_high, a_low, z_all, z_turned, z_both, m_high, m_low,
    rows, near0, near12, offset, parts_in, half_in, sums, plain, far0, far1,
    in_sems, raw_sems, send_sems, recv0, recv12, z_send, z_recv,
    part_send, part_recv, half_send, half_recv, sum_send, sum_recv, ready,
):
    group = slices // 2
    zed = lax.axis_index("tm")
    me = lax.axis_index("sub")

    far0[...] = jnp.zeros_like(far0)
    far1[...] = jnp.zeros_like(far1)
    plain[...] = jnp.zeros_like(plain)

    pairs = (
        (starts_h, starts), (block_h, block), (retain_h, retain), (sources_h, sources),
        (partner_h, partner), (admittance_h, admittance), (live_h, live), (delay_h, delay),
        (decay_h, decay),
    )
    loads = [pltpu.make_async_copy(a, b, in_sems.at[k]) for k, (a, b) in enumerate(pairs)]
    depth = NODES // CHUNKS
    chunks = [
        pltpu.make_async_copy(
            inverses_h.at[pl.ds(k * depth, depth), :], raw.at[pl.ds(k * depth, depth), :],
            raw_sems.at[k],
        )
        for k in range(CHUNKS)
    ]
    for load in loads:
        load.start()
    for chunk in chunks:
        chunk.start()
    barrier = pltpu.get_barrier_semaphore()

    @pl.loop(1, subs)
    def _(o):
        pl.semaphore_signal(
            barrier, inc=1, device_id={"sub": lax.rem(me + o, subs)}, device_id_type=MESH
        )

    @pl.loop(1, slices)
    def _(o):
        @pl.when(zed + o < slices)
        def _():
            pl.semaphore_signal(
                barrier, inc=1, device_id={"tm": lax.rem(zed + o, slices)}, device_id_type=MESH
            )

    for load in loads:
        load.wait()

    gain = retain[...]
    inverse_gain = 1.0 / gain
    lane = lax.broadcasted_iota(jnp.int32, (LINES, NODES), 1)
    slot = lax.broadcasted_iota(jnp.int32, (LINES, NODES), 0)
    first = jnp.zeros((LINES, NODES), jnp.int32)
    for l in range(LINES):
        first = jnp.where(slot == l, block[0, l] * TERM, first)
    ones = [(lane == first + t).astype(F32) for t in range(TERM)]
    inputs = jnp.concatenate(
        [
            starts[...],
            sources[...] * inverse_gain,
            jnp.zeros((COLS, NODES), F32),
            jnp.broadcast_to(inverse_gain, (COLS, NODES)),
        ]
        + ones,
        axis=0,
    )
    turned = jnp.transpose(inputs)
    z_all[0] = turned.reshape(NODES // TERM, TERM, LANES)

    def pick(at):
        for l in range(LINES):
            rows[at, pl.ds(l * TERM, TERM), :] = z_all[at, block[0, l]]

    pick(0)
    near0[me] = packed(rows, 0, 0)

    pl.semaphore_wait(barrier, subs - 1 + zed)

    @pl.loop(1, slices)
    def _(o):
        @pl.when(zed >= o)
        def _():
            pl.semaphore_signal(
                ready.at[zed], inc=1, device_id={"tm": lax.rem(zed + slices - o, slices)},
                device_id_type=MESH,
            )

    def sub_copy(ref, send, recv, o):
        return pltpu.make_async_remote_copy(
            src_ref=ref.at[me], dst_ref=ref.at[me], send_sem=send, recv_sem=recv,
            device_id={"sub": lax.rem(me + o, subs)}, device_id_type=MESH,
        )

    def all_of(ref, send, recv):
        whole = ref.at[pl.ds(0, subs - 1)]
        return pltpu.make_async_remote_copy(
            src_ref=whole, dst_ref=whole, send_sem=send, recv_sem=recv,
            device_id={"sub": lax.rem(me + 1, subs)}, device_id_type=MESH,
        )

    @pl.loop(1, subs)
    def _(o):
        sub_copy(near0, send_sems.at[0], recv0, o).start()

    slot8 = lax.broadcasted_iota(jnp.int32, (LINES, LANES), 0)
    weight = jnp.zeros((LINES, LANES), F32)
    for l in range(LINES):
        weight = jnp.where(slot8 == l, admittance[0, l] * live[0, l].astype(F32), weight)
    weight = weight * packed(rows, 0, 3 * COLS)

    high, low = split(turned)
    z_both[:, :LANES] = high
    z_both[:, LANES:] = low
    for k in range(CHUNKS):
        chunks[k].wait()
        piece = pl.ds(k * depth, depth)
        high, low = split(raw[piece, :] * gain)
        a_high[piece, :] = high
        a_low[piece, :] = low

    def advance(k):
        both = z_both[...]
        y = dot(a_high[...], both) + dot(a_low[...], both)
        new = y[:, :LANES] + y[:, LANES:]
        z_all[k] = new.reshape(NODES // TERM, TERM, LANES)
        high, low = split(new)
        z_both[:, :LANES] = high
        z_both[:, LANES:] = low
        z_turned[k - 1] = jnp.transpose(new)

    @pl.loop(1, 4)
    def _(k):
        advance(k)

    pick(1)
    pick(2)
    lanes64 = lax.broadcasted_iota(jnp.int32, (LINES * TERM, LANES), 1)
    first_rows = rows[1]
    second_rows = rows[2] + jnp.where(lanes64 >= COLS, first_rows, 0.0)
    q_high, q_low = split(jnp.concatenate([first_rows, second_rows], axis=0))
    q_both = jnp.concatenate([q_high, q_low], axis=1)
    r32 = lax.broadcasted_iota(jnp.int32, (4 * COLS, LANES), 0)
    c32 = lax.broadcasted_iota(jnp.int32, (4 * COLS, LANES), 1)
    unit = jnp.where(
        (c32 < COLS) & (r32 < 2 * COLS) & ((r32 == c32) | (r32 == c32 + COLS)), 1.0, 0.0
    ).astype(F32)

    all_of(near0, send_sems.at[0], recv0).wait_recv()
    def row_of(tile, l):
        return jnp.sum(jnp.where(slot8 == lax.rem(partner[0, l], LINES), tile, 0.0), axis=0, keepdims=True)

    olds = jnp.zeros((LINES, LANES), F32)
    for l in range(LINES):
        olds = jnp.where(slot8 == l, row_of(near0[lax.div(partner[0, l], LINES)], l), olds)
    spread0 = unpacked(olds * weight)
    e_high, e_low = split(jnp.concatenate([unit, spread0], axis=0))
    e_both = jnp.concatenate([e_high, e_low], axis=1)
    e_both = jnp.concatenate([e_both, e_both], axis=0)
    s = dot(q_both, e_both)
    s = s[:, :LANES] + s[:, LANES:]
    rows[1] = s[: LINES * TERM]
    rows[2] = s[LINES * TERM :]
    near12[me, 0] = packed(rows, 1, 0)
    near12[me, 1] = packed(rows, 2, 0)

    @pl.loop(1, subs)
    def _(o):
        sub_copy(near12, send_sems.at[1], recv12, o).start()

    advance(4)

    mine_z = pl.ds(pl.multiple_of(zed * COLS, COLS), COLS)
    base = z_turned[3, :COLS, :]
    for k in range(4):
        base = base + z_turned[k, COLS : 2 * COLS, :]
    slope = decay[...]
    base = jnp.where(zed == 0, base, base - slope * starts[...])
    width = NODES // group
    for k in range(group):
        offset[k] = base[:, k * width : (k + 1) * width]
    side = lax.div(zed, group)
    place = lax.rem(zed, group)
    half_in[place] = offset[...]
    parts_in[zed] = offset[place]

    def half_copy(to, sender):
        return pltpu.make_async_remote_copy(
            src_ref=offset, dst_ref=half_in.at[place],
            send_sem=half_send.at[to], recv_sem=half_recv.at[sender],
            device_id={"tm": side * group + to}, device_id_type=MESH,
        )

    def part_copy(to, sender):
        return pltpu.make_async_remote_copy(
            src_ref=offset.at[to], dst_ref=parts_in.at[zed],
            send_sem=part_send.at[to], recv_sem=part_recv.at[sender],
            device_id={"tm": group + to}, device_id_type=MESH,
        )

    def sum_copy(to, owner):
        return pltpu.make_async_remote_copy(
            src_ref=sums.at[to], dst_ref=plain.at[place],
            send_sem=sum_send.at[to], recv_sem=sum_recv.at[owner],
            device_id={"tm": group + to}, device_id_type=MESH,
        )

    @pl.loop(0, group)
    def _(to):
        @pl.when(zed < group + to)
        def _():
            pl.semaphore_wait(ready.at[group + to], 1)

        @pl.when(zed != group + to)
        def _():
            part_copy(to, zed).start()

    @pl.when(side == 0)
    def _():
        @pl.loop(0, group)
        def _(to):
            @pl.when(to > place)
            def _():
                pl.semaphore_wait(ready.at[to], 1)
                half_copy(to, place).start()

    def z_copy(ref, which, d):
        return pltpu.make_async_remote_copy(
            src_ref=ref.at[mine_z, :], dst_ref=ref.at[mine_z, :],
            send_sem=z_send.at[which, d], recv_sem=z_recv.at[which, d],
            device_id={"tm": lax.rem(zed + d, slices)}, device_id_type=MESH,
        )

    def z_start(ref, which):
        @pl.loop(1, slices)
        def _(d):
            @pl.when(zed + d < slices)
            def _():
                z_copy(ref, which, d).start()

    def z_arrive(ref, which):
        @pl.loop(1, slices)
        def _(d):
            @pl.when(zed >= d)
            def _():
                z_copy(ref, which, d).wait_recv()

    def z_sent(ref, which):
        @pl.loop(1, slices)
        def _(d):
            @pl.when(zed + d < slices)
            def _():
                z_copy(ref, which, d).wait_send()

    blank = jnp.zeros((LINES * TERM, LANES), F32)
    far0[mine_z, :] = jnp.transpose(jnp.concatenate([spread0, blank], axis=0))[:COLS]
    z_start(far0, 0)

    half = LINES * TERM
    effect = jnp.concatenate(
        [
            z_turned[2, half:, :] + z_turned[3, half:, :],
            jnp.zeros((half, NODES), F32),
            z_turned[1, half:, :],
            z_turned[0, half:, :],
        ],
        axis=0,
    )
    high, low = split(effect)
    m_high[...] = high
    m_low[...] = low

    all_of(near12, send_sems.at[1], recv12).wait_recv()
    fars = []
    for step in (2, 3):
        far = olds
        for l in range(LINES):
            reach = step + 1 - delay[0, l]
            late = jnp.minimum(jnp.maximum(reach, 1), 2) - 1
            row = row_of(near12[lax.div(partner[0, l], LINES), late], l)
            far = jnp.where((slot8 == l) & (jnp.full((LINES, LANES), reach, jnp.int32) > 0), row, far)
        fars.append(unpacked(far * weight))
    spread = jnp.concatenate(fars, axis=0)
    far1[mine_z, :] = jnp.transpose(spread)[:COLS]
    z_start(far1, 1)

    @pl.when(side == 1)
    def _():
        @pl.loop(0, slices)
        def _(sender):
            @pl.when(sender != zed)
            def _():
                part_copy(place, sender).wait_recv()

        bend = decay[:, pl.ds(pl.multiple_of(place * width, LANES), width)]
        state = parts_in[0]
        for k in range(1, slices):
            state = bend * state + parts_in[k]
            if k >= group:
                sums[k - group] = state
        plain[place] = sums[place]

        @pl.loop(0, group)
        def _(to):
            @pl.when(to != place)
            def _():
                sum_copy(to, place).start()

        @pl.loop(0, group)
        def _(owner):
            @pl.when(owner != place)
            def _():
                sum_copy(owner, owner).wait_recv()

    @pl.when(side == 0)
    def _():
        @pl.loop(0, group)
        def _(sender):
            @pl.when(sender < place)
            def _():
                half_copy(sender, sender).wait_recv()

    bends = [slope[:, k * width : (k + 1) * width] for k in range(group)]

    def one(i, states):
        return tuple(bends[k] * states[k] + half_in[i, k] for k in range(group))

    steps = jnp.where(side == 0, place + 1, 0)
    summed = lax.fori_loop(0, steps, one, tuple(plain[k] for k in range(group)))

    z_arrive(far0, 0)
    z_arrive(far1, 1)
    high, low = split(jnp.concatenate([far0[...], far1[...]], axis=1))
    count = slices * COLS
    y = dot(jnp.concatenate([high, low], axis=0), m_high[...])
    y = y[:count] + y[count:] + dot(high, m_low[...])
    state = jnp.zeros((COLS, NODES), F32)
    for i in range(slices):
        state = jnp.where(i <= zed, slope * state + y[i * COLS : (i + 1) * COLS], state)
    for k in range(group):
        part = slice(k * width, (k + 1) * width)
        out_ref[:, part] = summed[k] + state[:, part]

    all_of(near0, send_sems.at[0], recv0).wait_send()
    all_of(near12, send_sems.at[1], recv12).wait_send()

    @pl.loop(0, group)
    def _(to):
        @pl.when(zed != group + to)
        def _():
            part_copy(to, zed).wait_send()

        @pl.when((side == 0) & (to > place))
        def _():
            half_copy(to, place).wait_send()

        @pl.when((side == 1) & (to != place))
        def _():
            sum_copy(to, place).wait_send()

    z_sent(far0, 0)
    z_sent(far1, 1)


def shards(slices, subs, starts, inverses, retain, sources, decay, admittance, partner, delay, live, block):
    vmem, smem = pltpu.VMEM, pltpu.SMEM
    group = slices // 2
    out = pl.pallas_call(
        functools.partial(kernel, slices, subs),
        out_shape=jax.ShapeDtypeStruct((COLS, NODES), F32),
        in_specs=[pl.BlockSpec(memory_space=pltpu.HBM)] * 10,
        out_specs=pl.BlockSpec(memory_space=pltpu.VMEM),
        scratch_shapes=[
            vmem((COLS, NODES), F32), vmem((COLS, NODES), F32),
            vmem((1, NODES), F32), vmem((1, NODES), F32),
            smem((1, LINES), F32), smem((1, LINES), jnp.int32), smem((1, LINES), jnp.int32),
            smem((1, LINES), jnp.int32), smem((1, LINES), jnp.int32),
            vmem((NODES, NODES), F32), vmem((NODES, NODES), BF16), vmem((NODES, NODES), BF16),
            vmem((5, NODES // TERM, TERM, LANES), F32), vmem((4, LANES, NODES), F32),
            vmem((NODES, 2 * LANES), BF16),
            vmem((2 * LANES, NODES), BF16), vmem((2 * LANES, NODES), BF16),
            vmem((3, LINES * TERM, LANES), F32),
            vmem((subs, LINES, LANES), F32), vmem((subs, 2, LINES, LANES), F32),
            vmem((group, COLS, NODES // group), F32), vmem((slices, COLS, NODES // group), F32),
            vmem((group, group, COLS, NODES // group), F32),
            vmem((group, COLS, NODES // group), F32), vmem((group, COLS, NODES // group), F32),
            vmem((slices * COLS, LANES), F32), vmem((slices * COLS, LANES), F32),
            pltpu.SemaphoreType.DMA((9,)), pltpu.SemaphoreType.DMA((CHUNKS,)),
            pltpu.SemaphoreType.DMA((2,)), pltpu.SemaphoreType.DMA, pltpu.SemaphoreType.DMA,
            pltpu.SemaphoreType.DMA((2, slices)), pltpu.SemaphoreType.DMA((2, slices)),
            pltpu.SemaphoreType.DMA((group,)), pltpu.SemaphoreType.DMA((slices,)),
            pltpu.SemaphoreType.DMA((group,)), pltpu.SemaphoreType.DMA((group,)),
            pltpu.SemaphoreType.DMA((group,)), pltpu.SemaphoreType.DMA((group,)),
            pltpu.SemaphoreType.REGULAR((slices,)),
        ],
        compiler_params=pltpu.CompilerParams(
            collective_id=0, has_side_effects=True, vmem_limit_bytes=48 * 1024 * 1024
        ),
    )(*[pltpu.with_memory_space_constraint(a, pltpu.HBM) for a in (
        starts.reshape(COLS, NODES), inverses.reshape(NODES, NODES), retain,
        sources.reshape(COLS, NODES), decay, admittance, partner, delay, live, block,
    )])
    return out.reshape(1, 1, COLS, NODES)


def solution(mesh):
    return jax.shard_map(
        functools.partial(shards, mesh.shape["tm"], mesh.shape["sub"]),
        mesh=mesh,
        in_specs=(
            P("tm", "sub", None, None),
            P("sub", None, None),
            P("sub", None),
            P("sub", None, None),
            P("sub", None),
            P("sub", None),
            P("sub", None),
            P("sub", None),
            P("sub", None),
            P("sub", None),
        ),
        out_specs=P("tm", "sub", None, None),
        check_vma=False,
    )
```

```python
import functools

import jax
import jax.numpy as jnp
from jax import lax
from jax.experimental import pallas as pl
from jax.experimental.pallas import tpu as pltpu
from jax.sharding import PartitionSpec as P

TERM = 8
LINES = 8
COLS = 16
LANES = 128
NODES = 1024
CHUNKS = 8
MESH = pl.DeviceIdType.MESH
F32 = jnp.float32
BF16 = jnp.bfloat16


def split(x):
    high = x.astype(BF16)
    low = (x - high.astype(F32)).astype(BF16)
    return high, low


def dot(a, b):
    return jnp.dot(a, b, preferred_element_type=F32)


def packed(ref, at, offset):
    group = lax.broadcasted_iota(jnp.int32, (LINES, LANES), 1) // COLS
    out = jnp.zeros((LINES, LANES), F32)
    for t in range(TERM):
        rows = ref[at, pl.ds(t, LINES, stride=TERM), :]
        shift = (COLS * t - offset) % LANES
        rows = pltpu.roll(rows, shift, 1) if shift else rows
        out = jnp.where(group == t, rows, out)
    return out


def unpacked(far):
    return jnp.concatenate(
        [far] + [pltpu.roll(far, LANES - COLS * t, 1) for t in range(1, TERM)], axis=0
    )


def far_first(me, subs):
    if subs != 32:
        return [lax.rem(me + o, subs) for o in range(1, subs)]
    rows = [8 * ((lax.div(me, 8) + d) & 3) for d in range(4)]
    columns = [2 * ((lax.div(me, 2) + d) & 3) for d in range(4)]
    cores = [(me + d) & 1 for d in range(2)]
    apart = [(y, x, core) for core in range(2) for y in range(4) for x in range(4)][1:]
    hops = lambda d: min(d, 4 - d)
    apart.sort(key=lambda d: -(hops(d[0]) + hops(d[1])))
    return [rows[y] + columns[x] + cores[core] for y, x, core in apart]


def hops_of(me, subs):
    if subs != 32:
        return me
    row, column = lax.div(me, 8) & 3, lax.div(me, 2) & 3
    return jnp.minimum(row, 4 - row) + jnp.minimum(column, 4 - column)


def kernel(
    slices, subs,
    starts_h, inverses_h, retain_h, sources_h, decay_h,
    admittance_h, partner_h, delay_h, live_h, block_h,
    out_ref,
    starts, sources, retain, decay, admittance, partner, delay, live, block,
    raw, a_high, a_low, z_all, z_turned, z_both, m_high, m_low,
    rows, near0, near12, offset, parts_in, half_in, sums, plain, far0, far1,
    in_sems, raw_sems, send_sems, recv0, recv12, z_send, z_recv,
    part_send, part_recv, half_send, half_recv, sum_send, sum_recv, ready,
):
    group = slices // 2
    zed = lax.axis_index("tm")
    me = lax.axis_index("sub")

    far0[...] = jnp.zeros_like(far0)
    far1[...] = jnp.zeros_like(far1)
    plain[...] = jnp.zeros_like(plain)

    pairs = (
        (starts_h, starts), (block_h, block), (retain_h, retain), (sources_h, sources),
        (partner_h, partner), (admittance_h, admittance), (live_h, live), (delay_h, delay),
        (decay_h, decay),
    )
    loads = [pltpu.make_async_copy(a, b, in_sems.at[k]) for k, (a, b) in enumerate(pairs)]
    depth = NODES // CHUNKS
    chunks = [
        pltpu.make_async_copy(
            inverses_h.at[pl.ds(k * depth, depth), :], raw.at[pl.ds(k * depth, depth), :],
            raw_sems.at[k],
        )
        for k in range(CHUNKS)
    ]
    for load in loads:
        load.start()
    for chunk in chunks:
        chunk.start()
    barrier = pltpu.get_barrier_semaphore()

    others = far_first(me, subs)
    for other in others:
        pl.semaphore_signal(barrier, inc=1, device_id={"sub": other}, device_id_type=MESH)

    @pl.loop(1, slices)
    def _(o):
        @pl.when(zed + o < slices)
        def _():
            pl.semaphore_signal(
                barrier, inc=1, device_id={"tm": lax.rem(zed + o, slices)}, device_id_type=MESH
            )

    for load in loads:
        load.wait()

    gain = retain[...]
    inverse_gain = 1.0 / gain
    lane = lax.broadcasted_iota(jnp.int32, (LINES, NODES), 1)
    slot = lax.broadcasted_iota(jnp.int32, (LINES, NODES), 0)
    first = jnp.zeros((LINES, NODES), jnp.int32)
    for l in range(LINES):
        first = jnp.where(slot == l, block[0, l] * TERM, first)
    ones = [(lane == first + t).astype(F32) for t in range(TERM)]
    inputs = jnp.concatenate(
        [
            starts[...],
            sources[...] * inverse_gain,
            jnp.zeros((COLS, NODES), F32),
            jnp.broadcast_to(inverse_gain, (COLS, NODES)),
        ]
        + ones,
        axis=0,
    )
    turned = jnp.transpose(inputs)
    z_all[0] = turned.reshape(NODES // TERM, TERM, LANES)

    def pick(at):
        for l in range(LINES):
            rows[at, pl.ds(l * TERM, TERM), :] = z_all[at, block[0, l]]

    pick(0)
    near0[me] = packed(rows, 0, 0)

    high, low = split(turned)
    z_both[:, :LANES] = high
    z_both[:, LANES:] = low

    def divide():
        for k in range(CHUNKS):
            chunks[k].wait()
            piece = pl.ds(k * depth, depth)
            high, low = split(raw[piece, :] * gain)
            a_high[piece, :] = high
            a_low[piece, :] = low

    def advance(k, carry):
        both = z_both[...]
        y = dot(a_high[...], both) + dot(a_low[...], both)
        new = y[:, :LANES] + y[:, LANES:]
        z_all[k] = new.reshape(NODES // TERM, TERM, LANES)
        high, low = split(new)
        z_both[:, :LANES] = high
        z_both[:, LANES:] = low
        z_turned[k - 1] = jnp.transpose(new)
        return carry

    hops = hops_of(me, subs)
    ahead = jnp.maximum(1 - hops, 0)

    @pl.when(hops < 4)
    def _():
        divide()

    lax.fori_loop(1, 1 + ahead, advance, 0)

    pl.semaphore_wait(barrier, subs - 1 + zed)

    def sub_copy(ref, send, recv, other):
        return pltpu.make_async_remote_copy(
            src_ref=ref.at[me], dst_ref=ref.at[me], send_sem=send, recv_sem=recv,
            device_id={"sub": other}, device_id_type=MESH,
        )

    def all_of(ref, send, recv):
        whole = ref.at[pl.ds(0, subs - 1)]
        return pltpu.make_async_remote_copy(
            src_ref=whole, dst_ref=whole, send_sem=send, recv_sem=recv,
            device_id={"sub": lax.rem(me + 1, subs)}, device_id_type=MESH,
        )

    for other in others:
        sub_copy(near0, send_sems.at[0], recv0, other).start()

    @pl.loop(1, slices)
    def _(o):
        @pl.when(zed >= o)
        def _():
            pl.semaphore_signal(
                ready.at[zed], inc=1, device_id={"tm": lax.rem(zed + slices - o, slices)},
                device_id_type=MESH,
            )

    slot8 = lax.broadcasted_iota(jnp.int32, (LINES, LANES), 0)
    weight = jnp.zeros((LINES, LANES), F32)
    for l in range(LINES):
        weight = jnp.where(slot8 == l, admittance[0, l] * live[0, l].astype(F32), weight)
    weight = weight * packed(rows, 0, 3 * COLS)

    @pl.when(hops >= 4)
    def _():
        divide()

    lax.fori_loop(1 + ahead, 5, advance, 0)

    mine_z = pl.ds(pl.multiple_of(zed * COLS, COLS), COLS)
    base = z_turned[3, :COLS, :]
    for k in range(4):
        base = base + z_turned[k, COLS : 2 * COLS, :]
    slope = decay[...]
    base = jnp.where(zed == 0, base, base - slope * starts[...])
    width = NODES // group
    for k in range(group):
        offset[k] = base[:, k * width : (k + 1) * width]
    side = lax.div(zed, group)
    place = lax.rem(zed, group)
    half_in[place] = offset[...]
    parts_in[zed] = offset[place]

    def half_copy(to, sender):
        return pltpu.make_async_remote_copy(
            src_ref=offset, dst_ref=half_in.at[place],
            send_sem=half_send.at[to], recv_sem=half_recv.at[sender],
            device_id={"tm": side * group + to}, device_id_type=MESH,
        )

    def part_copy(to, sender):
        return pltpu.make_async_remote_copy(
            src_ref=offset.at[to], dst_ref=parts_in.at[zed],
            send_sem=part_send.at[to], recv_sem=part_recv.at[sender],
            device_id={"tm": group + to}, device_id_type=MESH,
        )

    def sum_copy(to, owner):
        return pltpu.make_async_remote_copy(
            src_ref=sums.at[to], dst_ref=plain.at[place],
            send_sem=sum_send.at[to], recv_sem=sum_recv.at[owner],
            device_id={"tm": group + to}, device_id_type=MESH,
        )

    def send_offsets():
        @pl.loop(0, group)
        def _(to):
            @pl.when(zed < group + to)
            def _():
                pl.semaphore_wait(ready.at[group + to], 1)

            @pl.when(zed != group + to)
            def _():
                part_copy(to, zed).start()

        @pl.when(side == 0)
        def _():
            @pl.loop(0, group)
            def _(to):
                @pl.when(to > place)
                def _():
                    pl.semaphore_wait(ready.at[to], 1)
                    half_copy(to, place).start()

    @pl.when(zed >= 2)
    def _():
        send_offsets()

    def z_copy(ref, which, d):
        return pltpu.make_async_remote_copy(
            src_ref=ref.at[mine_z, :], dst_ref=ref.at[mine_z, :],
            send_sem=z_send.at[which, d], recv_sem=z_recv.at[which, d],
            device_id={"tm": lax.rem(zed + d, slices)}, device_id_type=MESH,
        )

    def z_start(ref, which):
        @pl.loop(1, slices)
        def _(d):
            @pl.when(zed + d < slices)
            def _():
                z_copy(ref, which, d).start()

    def z_arrive(ref, which):
        @pl.loop(1, slices)
        def _(d):
            @pl.when(zed >= d)
            def _():
                z_copy(ref, which, d).wait_recv()

    def z_sent(ref, which):
        @pl.loop(1, slices)
        def _(d):
            @pl.when(zed + d < slices)
            def _():
                z_copy(ref, which, d).wait_send()

    pick(1)
    pick(2)
    lanes64 = lax.broadcasted_iota(jnp.int32, (LINES * TERM, LANES), 1)
    first_rows = rows[1]
    second_rows = rows[2] + jnp.where(lanes64 >= COLS, first_rows, 0.0)
    q_high, q_low = split(jnp.concatenate([first_rows, second_rows], axis=0))
    q_both = jnp.concatenate([q_high, q_low], axis=1)
    r32 = lax.broadcasted_iota(jnp.int32, (4 * COLS, LANES), 0)
    c32 = lax.broadcasted_iota(jnp.int32, (4 * COLS, LANES), 1)
    unit = jnp.where(
        (c32 < COLS) & (r32 < 2 * COLS) & ((r32 == c32) | (r32 == c32 + COLS)), 1.0, 0.0
    ).astype(F32)

    all_of(near0, send_sems.at[0], recv0).wait_recv()
    def row_of(tile, l):
        return jnp.sum(jnp.where(slot8 == lax.rem(partner[0, l], LINES), tile, 0.0), axis=0, keepdims=True)

    olds = jnp.zeros((LINES, LANES), F32)
    for l in range(LINES):
        olds = jnp.where(slot8 == l, row_of(near0[lax.div(partner[0, l], LINES)], l), olds)
    spread0 = unpacked(olds * weight)
    e_high, e_low = split(jnp.concatenate([unit, spread0], axis=0))
    e_both = jnp.concatenate([e_high, e_low], axis=1)
    e_both = jnp.concatenate([e_both, e_both], axis=0)
    s = dot(q_both, e_both)
    s = s[:, :LANES] + s[:, LANES:]
    rows[1] = s[: LINES * TERM]
    rows[2] = s[LINES * TERM :]
    near12[me, 0] = packed(rows, 1, 0)
    near12[me, 1] = packed(rows, 2, 0)

    for other in others:
        sub_copy(near12, send_sems.at[1], recv12, other).start()

    @pl.when(zed < 2)
    def _():
        send_offsets()

    blank = jnp.zeros((LINES * TERM, LANES), F32)
    far0[mine_z, :] = jnp.transpose(jnp.concatenate([spread0, blank], axis=0))[:COLS]
    z_start(far0, 0)

    half = LINES * TERM
    effect = jnp.concatenate(
        [
            z_turned[2, half:, :] + z_turned[3, half:, :],
            jnp.zeros((half, NODES), F32),
            z_turned[1, half:, :],
            z_turned[0, half:, :],
        ],
        axis=0,
    )
    high, low = split(effect)
    m_high[...] = high
    m_low[...] = low

    all_of(near12, send_sems.at[1], recv12).wait_recv()
    fars = []
    for step in (2, 3):
        far = olds
        for l in range(LINES):
            reach = step + 1 - delay[0, l]
            late = jnp.minimum(jnp.maximum(reach, 1), 2) - 1
            row = row_of(near12[lax.div(partner[0, l], LINES), late], l)
            far = jnp.where((slot8 == l) & (jnp.full((LINES, LANES), reach, jnp.int32) > 0), row, far)
        fars.append(unpacked(far * weight))
    spread = jnp.concatenate(fars, axis=0)
    far1[mine_z, :] = jnp.transpose(spread)[:COLS]
    z_start(far1, 1)

    @pl.when(side == 1)
    def _():
        @pl.loop(0, slices)
        def _(sender):
            @pl.when(sender != zed)
            def _():
                part_copy(place, sender).wait_recv()

        bend = decay[:, pl.ds(pl.multiple_of(place * width, LANES), width)]
        state = parts_in[0]
        for k in range(1, slices):
            state = bend * state + parts_in[k]
            if k >= group:
                sums[k - group] = state
        plain[place] = sums[place]

        @pl.loop(0, group)
        def _(to):
            @pl.when(to != place)
            def _():
                sum_copy(to, place).start()

        @pl.loop(0, group)
        def _(owner):
            @pl.when(owner != place)
            def _():
                sum_copy(owner, owner).wait_recv()

    @pl.when(side == 0)
    def _():
        @pl.loop(0, group)
        def _(sender):
            @pl.when(sender < place)
            def _():
                half_copy(sender, sender).wait_recv()

    bends = [slope[:, k * width : (k + 1) * width] for k in range(group)]

    def one(i, states):
        return tuple(bends[k] * states[k] + half_in[i, k] for k in range(group))

    steps = jnp.where(side == 0, place + 1, 0)
    summed = lax.fori_loop(0, steps, one, tuple(plain[k] for k in range(group)))

    z_arrive(far0, 0)
    z_arrive(far1, 1)
    high, low = split(jnp.concatenate([far0[...], far1[...]], axis=1))
    count = slices * COLS
    y = dot(jnp.concatenate([high, low], axis=0), m_high[...])
    y = y[:count] + y[count:] + dot(high, m_low[...])
    state = jnp.zeros((COLS, NODES), F32)
    for i in range(slices):
        state = jnp.where(i <= zed, slope * state + y[i * COLS : (i + 1) * COLS], state)
    for k in range(group):
        part = slice(k * width, (k + 1) * width)
        out_ref[:, part] = summed[k] + state[:, part]

    all_of(near0, send_sems.at[0], recv0).wait_send()
    all_of(near12, send_sems.at[1], recv12).wait_send()

    @pl.loop(0, group)
    def _(to):
        @pl.when(zed != group + to)
        def _():
            part_copy(to, zed).wait_send()

        @pl.when((side == 0) & (to > place))
        def _():
            half_copy(to, place).wait_send()

        @pl.when((side == 1) & (to != place))
        def _():
            sum_copy(to, place).wait_send()

    z_sent(far0, 0)
    z_sent(far1, 1)


def shards(slices, subs, starts, inverses, retain, sources, decay, admittance, partner, delay, live, block):
    vmem, smem = pltpu.VMEM, pltpu.SMEM
    group = slices // 2
    out = pl.pallas_call(
        functools.partial(kernel, slices, subs),
        out_shape=jax.ShapeDtypeStruct((COLS, NODES), F32),
        in_specs=[pl.BlockSpec(memory_space=pltpu.HBM)] * 10,
        out_specs=pl.BlockSpec(memory_space=pltpu.VMEM),
        scratch_shapes=[
            vmem((COLS, NODES), F32), vmem((COLS, NODES), F32),
            vmem((1, NODES), F32), vmem((1, NODES), F32),
            smem((1, LINES), F32), smem((1, LINES), jnp.int32), smem((1, LINES), jnp.int32),
            smem((1, LINES), jnp.int32), smem((1, LINES), jnp.int32),
            vmem((NODES, NODES), F32), vmem((NODES, NODES), BF16), vmem((NODES, NODES), BF16),
            vmem((5, NODES // TERM, TERM, LANES), F32), vmem((4, LANES, NODES), F32),
            vmem((NODES, 2 * LANES), BF16),
            vmem((2 * LANES, NODES), BF16), vmem((2 * LANES, NODES), BF16),
            vmem((3, LINES * TERM, LANES), F32),
            vmem((subs, LINES, LANES), F32), vmem((subs, 2, LINES, LANES), F32),
            vmem((group, COLS, NODES // group), F32), vmem((slices, COLS, NODES // group), F32),
            vmem((group, group, COLS, NODES // group), F32),
            vmem((group, COLS, NODES // group), F32), vmem((group, COLS, NODES // group), F32),
            vmem((slices * COLS, LANES), F32), vmem((slices * COLS, LANES), F32),
            pltpu.SemaphoreType.DMA((9,)), pltpu.SemaphoreType.DMA((CHUNKS,)),
            pltpu.SemaphoreType.DMA((2,)), pltpu.SemaphoreType.DMA, pltpu.SemaphoreType.DMA,
            pltpu.SemaphoreType.DMA((2, slices)), pltpu.SemaphoreType.DMA((2, slices)),
            pltpu.SemaphoreType.DMA((group,)), pltpu.SemaphoreType.DMA((slices,)),
            pltpu.SemaphoreType.DMA((group,)), pltpu.SemaphoreType.DMA((group,)),
            pltpu.SemaphoreType.DMA((group,)), pltpu.SemaphoreType.DMA((group,)),
            pltpu.SemaphoreType.REGULAR((slices,)),
        ],
        compiler_params=pltpu.CompilerParams(
            collective_id=0, has_side_effects=True, vmem_limit_bytes=48 * 1024 * 1024
        ),
    )(*[pltpu.with_memory_space_constraint(a, pltpu.HBM) for a in (
        starts.reshape(COLS, NODES), inverses.reshape(NODES, NODES), retain,
        sources.reshape(COLS, NODES), decay, admittance, partner, delay, live, block,
    )])
    return out.reshape(1, 1, COLS, NODES)


def solution(mesh):
    return jax.shard_map(
        functools.partial(shards, mesh.shape["tm"], mesh.shape["sub"]),
        mesh=mesh,
        in_specs=(
            P("tm", "sub", None, None),
            P("sub", None, None),
            P("sub", None),
            P("sub", None, None),
            P("sub", None),
            P("sub", None),
            P("sub", None),
            P("sub", None),
            P("sub", None),
            P("sub", None),
        ),
        out_specs=P("tm", "sub", None, None),
        check_vma=False,
    )
```

```python
import functools

import jax
import jax.numpy as jnp
from jax import lax
from jax.experimental import pallas as pl
from jax.experimental.pallas import tpu as pltpu
from jax.sharding import PartitionSpec as P

TERM = 8
LINES = 8
COLS = 16
LANES = 128
NODES = 1024
CHUNKS = 8
MESH = pl.DeviceIdType.MESH
F32 = jnp.float32
BF16 = jnp.bfloat16


def split(x):
    high = x.astype(BF16)
    low = (x - high.astype(F32)).astype(BF16)
    return high, low


def dot(a, b):
    return jnp.dot(a, b, preferred_element_type=F32)


def packed(ref, at, offset):
    group = lax.broadcasted_iota(jnp.int32, (LINES, LANES), 1) // COLS
    out = jnp.zeros((LINES, LANES), F32)
    for t in range(TERM):
        rows = ref[at, pl.ds(t, LINES, stride=TERM), :]
        shift = (COLS * t - offset) % LANES
        rows = pltpu.roll(rows, shift, 1) if shift else rows
        out = jnp.where(group == t, rows, out)
    return out


def unpacked(far):
    return jnp.concatenate(
        [far] + [pltpu.roll(far, LANES - COLS * t, 1) for t in range(1, TERM)], axis=0
    )


def far_first(me, subs):
    if subs != 32:
        return [lax.rem(me + o, subs) for o in range(1, subs)]
    rows = [8 * ((lax.div(me, 8) + d) & 3) for d in range(4)]
    columns = [2 * ((lax.div(me, 2) + d) & 3) for d in range(4)]
    cores = [(me + d) & 1 for d in range(2)]
    apart = [(y, x, core) for core in range(2) for y in range(4) for x in range(4)][1:]
    hops = lambda d: min(d, 4 - d)
    apart.sort(key=lambda d: -(hops(d[0]) + hops(d[1])))
    return [rows[y] + columns[x] + cores[core] for y, x, core in apart]


def hops_of(me, subs):
    if subs != 32:
        return me
    row, column = lax.div(me, 8) & 3, lax.div(me, 2) & 3
    return jnp.minimum(row, 4 - row) + jnp.minimum(column, 4 - column)


def kernel(
    slices, subs,
    starts_h, inverses_h, retain_h, sources_h, decay_h,
    admittance_h, partner_h, delay_h, live_h, block_h,
    out_ref,
    starts, sources, retain, decay, admittance, partner, delay, live, block,
    raw, a_high, a_low, z_all, z_turned, z_both, m_high, m_low,
    rows, near0, near12, offset, parts_in, half_in, sums, plain, far0, far1,
    in_sems, raw_sems, send_sems, recv0, recv12, z_send, z_recv,
    part_send, part_recv, half_send, half_recv, sum_send, sum_recv, ready,
):
    group = slices // 2
    zed = lax.axis_index("tm")
    me = lax.axis_index("sub")

    far0[...] = jnp.zeros_like(far0)
    far1[...] = jnp.zeros_like(far1)
    plain[...] = jnp.zeros_like(plain)

    pairs = (
        (starts_h, starts), (block_h, block), (retain_h, retain), (sources_h, sources),
        (partner_h, partner), (admittance_h, admittance), (live_h, live), (delay_h, delay),
        (decay_h, decay),
    )
    loads = [pltpu.make_async_copy(a, b, in_sems.at[k]) for k, (a, b) in enumerate(pairs)]
    depth = NODES // CHUNKS
    chunks = [
        pltpu.make_async_copy(
            inverses_h.at[pl.ds(k * depth, depth), :], raw.at[pl.ds(k * depth, depth), :],
            raw_sems.at[k],
        )
        for k in range(CHUNKS)
    ]
    for load in loads:
        load.start()
    for chunk in chunks:
        chunk.start()
    barrier = pltpu.get_barrier_semaphore()

    others = far_first(me, subs)
    for other in others:
        pl.semaphore_signal(barrier, inc=1, device_id={"sub": other}, device_id_type=MESH)

    @pl.loop(1, slices)
    def _(o):
        @pl.when(zed + o < slices)
        def _():
            pl.semaphore_signal(
                barrier, inc=1, device_id={"tm": lax.rem(zed + o, slices)}, device_id_type=MESH
            )

    for load in loads:
        load.wait()

    gain = retain[...]
    inverse_gain = 1.0 / gain
    lane = lax.broadcasted_iota(jnp.int32, (LINES, NODES), 1)
    slot = lax.broadcasted_iota(jnp.int32, (LINES, NODES), 0)
    first = jnp.zeros((LINES, NODES), jnp.int32)
    for l in range(LINES):
        first = jnp.where(slot == l, block[0, l] * TERM, first)
    ones = [(lane == first + t).astype(F32) for t in range(TERM)]
    inputs = jnp.concatenate(
        [
            starts[...],
            sources[...] * inverse_gain,
            jnp.zeros((COLS, NODES), F32),
            jnp.broadcast_to(inverse_gain, (COLS, NODES)),
        ]
        + ones,
        axis=0,
    )
    turned = jnp.transpose(inputs)
    z_all[0] = turned.reshape(NODES // TERM, TERM, LANES)

    def pick(at):
        for l in range(LINES):
            rows[at, pl.ds(l * TERM, TERM), :] = z_all[at, block[0, l]]

    pick(0)
    near0[me] = packed(rows, 0, 0)

    high, low = split(turned)
    z_both[:, :LANES] = high
    z_both[:, LANES:] = low

    def divide():
        for k in range(CHUNKS):
            chunks[k].wait()
            piece = pl.ds(k * depth, depth)
            high, low = split(raw[piece, :] * gain)
            a_high[piece, :] = high
            a_low[piece, :] = low

    def advance(k, carry):
        both = z_both[...]
        y = dot(a_high[...], both) + dot(a_low[...], both)
        new = y[:, :LANES] + y[:, LANES:]
        z_all[k] = new.reshape(NODES // TERM, TERM, LANES)
        high, low = split(new)
        z_both[:, :LANES] = high
        z_both[:, LANES:] = low
        z_turned[k - 1] = jnp.transpose(new)
        return carry

    hops = hops_of(me, subs)
    ahead = jnp.maximum(1 - hops, 0)

    @pl.when(hops < 4)
    def _():
        divide()

    lax.fori_loop(1, 1 + ahead, advance, 0)

    pl.semaphore_wait(barrier, subs - 1 + zed)

    def sub_copy(ref, send, recv, other):
        return pltpu.make_async_remote_copy(
            src_ref=ref.at[me], dst_ref=ref.at[me], send_sem=send, recv_sem=recv,
            device_id={"sub": other}, device_id_type=MESH,
        )

    def all_of(ref, send, recv):
        whole = ref.at[pl.ds(0, subs - 1)]
        return pltpu.make_async_remote_copy(
            src_ref=whole, dst_ref=whole, send_sem=send, recv_sem=recv,
            device_id={"sub": lax.rem(me + 1, subs)}, device_id_type=MESH,
        )

    for other in others:
        sub_copy(near0, send_sems.at[0], recv0, other).start()

    @pl.loop(1, slices)
    def _(o):
        @pl.when(zed >= o)
        def _():
            pl.semaphore_signal(
                ready.at[zed], inc=1, device_id={"tm": lax.rem(zed + slices - o, slices)},
                device_id_type=MESH,
            )

    slot8 = lax.broadcasted_iota(jnp.int32, (LINES, LANES), 0)
    weight = jnp.zeros((LINES, LANES), F32)
    for l in range(LINES):
        weight = jnp.where(slot8 == l, admittance[0, l] * live[0, l].astype(F32), weight)
    weight = weight * packed(rows, 0, 3 * COLS)

    @pl.when(hops >= 4)
    def _():
        divide()

    lax.fori_loop(1 + ahead, 5, advance, 0)

    mine_z = pl.ds(pl.multiple_of(zed * COLS, COLS), COLS)
    base = z_turned[3, :COLS, :]
    for k in range(4):
        base = base + z_turned[k, COLS : 2 * COLS, :]
    slope = decay[...]
    base = jnp.where(zed == 0, base, base - slope * starts[...])
    width = NODES // group
    for k in range(group):
        offset[k] = base[:, k * width : (k + 1) * width]
    side = lax.div(zed, group)
    place = lax.rem(zed, group)
    half_in[place] = offset[...]
    parts_in[zed] = offset[place]

    def half_copy(to, sender):
        return pltpu.make_async_remote_copy(
            src_ref=offset, dst_ref=half_in.at[place],
            send_sem=half_send.at[to], recv_sem=half_recv.at[sender],
            device_id={"tm": side * group + to}, device_id_type=MESH,
        )

    def part_copy(to, sender):
        return pltpu.make_async_remote_copy(
            src_ref=offset.at[to], dst_ref=parts_in.at[zed],
            send_sem=part_send.at[to], recv_sem=part_recv.at[sender],
            device_id={"tm": group + to}, device_id_type=MESH,
        )

    def sum_copy(to, owner):
        return pltpu.make_async_remote_copy(
            src_ref=sums.at[to], dst_ref=plain.at[place],
            send_sem=sum_send.at[to], recv_sem=sum_recv.at[owner],
            device_id={"tm": group + to}, device_id_type=MESH,
        )

    def send_offsets():
        @pl.loop(0, group)
        def _(to):
            @pl.when(zed < group + to)
            def _():
                pl.semaphore_wait(ready.at[group + to], 1)

            @pl.when(zed != group + to)
            def _():
                part_copy(to, zed).start()

        @pl.when(side == 0)
        def _():
            @pl.loop(0, group)
            def _(to):
                @pl.when(to > place)
                def _():
                    pl.semaphore_wait(ready.at[to], 1)
                    half_copy(to, place).start()

    @pl.when(zed >= 2)
    def _():
        send_offsets()

    def z_copy(ref, which, d):
        return pltpu.make_async_remote_copy(
            src_ref=ref.at[mine_z, :], dst_ref=ref.at[mine_z, :],
            send_sem=z_send.at[which, d], recv_sem=z_recv.at[which, d],
            device_id={"tm": lax.rem(zed + d, slices)}, device_id_type=MESH,
        )

    def z_start(ref, which):
        @pl.loop(1, slices)
        def _(d):
            @pl.when(zed + d < slices)
            def _():
                z_copy(ref, which, d).start()

    def z_arrive(ref, which):
        @pl.loop(1, slices)
        def _(d):
            @pl.when(zed >= d)
            def _():
                z_copy(ref, which, d).wait_recv()

    def z_sent(ref, which):
        @pl.loop(1, slices)
        def _(d):
            @pl.when(zed + d < slices)
            def _():
                z_copy(ref, which, d).wait_send()

    pick(1)
    pick(2)
    lanes64 = lax.broadcasted_iota(jnp.int32, (LINES * TERM, LANES), 1)
    first_rows = rows[1]
    second_rows = rows[2] + jnp.where(lanes64 >= COLS, first_rows, 0.0)
    q_high, q_low = split(jnp.concatenate([first_rows, second_rows], axis=0))
    q_both = jnp.concatenate([q_high, q_low], axis=1)
    r32 = lax.broadcasted_iota(jnp.int32, (4 * COLS, LANES), 0)
    c32 = lax.broadcasted_iota(jnp.int32, (4 * COLS, LANES), 1)
    unit = jnp.where(
        (c32 < COLS) & (r32 < 2 * COLS) & ((r32 == c32) | (r32 == c32 + COLS)), 1.0, 0.0
    ).astype(F32)

    all_of(near0, send_sems.at[0], recv0).wait_recv()
    def row_of(tile, l):
        return jnp.sum(jnp.where(slot8 == lax.rem(partner[0, l], LINES), tile, 0.0), axis=0, keepdims=True)

    olds = jnp.zeros((LINES, LANES), F32)
    for l in range(LINES):
        olds = jnp.where(slot8 == l, row_of(near0[lax.div(partner[0, l], LINES)], l), olds)
    spread0 = unpacked(olds * weight)
    e_high, e_low = split(jnp.concatenate([unit, spread0], axis=0))
    e_both = jnp.concatenate([e_high, e_low], axis=1)
    e_both = jnp.concatenate([e_both, e_both], axis=0)
    s = dot(q_both, e_both)
    s = s[:, :LANES] + s[:, LANES:]
    rows[1] = s[: LINES * TERM]
    rows[2] = s[LINES * TERM :]
    near12[me, 0] = packed(rows, 1, 0)
    near12[me, 1] = packed(rows, 2, 0)

    for other in others:
        sub_copy(near12, send_sems.at[1], recv12, other).start()

    @pl.when(zed < 2)
    def _():
        send_offsets()

    blank = jnp.zeros((LINES * TERM, LANES), F32)
    far0[mine_z, :] = jnp.transpose(jnp.concatenate([spread0, blank], axis=0))[:COLS]
    z_start(far0, 0)

    half = LINES * TERM
    effect = jnp.concatenate(
        [
            z_turned[2, half:, :] + z_turned[3, half:, :],
            jnp.zeros((half, NODES), F32),
            z_turned[1, half:, :],
            z_turned[0, half:, :],
        ],
        axis=0,
    )
    high, low = split(effect)
    m_high[...] = high
    m_low[...] = low

    @pl.when(side == 1)
    def _():
        @pl.loop(0, slices)
        def _(sender):
            @pl.when(sender != zed)
            def _():
                part_copy(place, sender).wait_recv()

        bend = decay[:, pl.ds(pl.multiple_of(place * width, LANES), width)]
        state = parts_in[0]
        for k in range(1, slices):
            state = bend * state + parts_in[k]
            if k >= group:
                sums[k - group] = state
        plain[place] = sums[place]

        @pl.loop(0, group)
        def _(to):
            @pl.when(to != place)
            def _():
                sum_copy(to, place).start()

    all_of(near12, send_sems.at[1], recv12).wait_recv()
    fars = []
    for step in (2, 3):
        far = olds
        for l in range(LINES):
            reach = step + 1 - delay[0, l]
            late = jnp.minimum(jnp.maximum(reach, 1), 2) - 1
            row = row_of(near12[lax.div(partner[0, l], LINES), late], l)
            far = jnp.where((slot8 == l) & (jnp.full((LINES, LANES), reach, jnp.int32) > 0), row, far)
        fars.append(unpacked(far * weight))
    spread = jnp.concatenate(fars, axis=0)
    far1[mine_z, :] = jnp.transpose(spread)[:COLS]
    z_start(far1, 1)

    @pl.when(side == 1)
    def _():
        @pl.loop(0, group)
        def _(owner):
            @pl.when(owner != place)
            def _():
                sum_copy(owner, owner).wait_recv()

    @pl.when(side == 0)
    def _():
        @pl.loop(0, group)
        def _(sender):
            @pl.when(sender < place)
            def _():
                half_copy(sender, sender).wait_recv()

    bends = [slope[:, k * width : (k + 1) * width] for k in range(group)]

    def one(i, states):
        return tuple(bends[k] * states[k] + half_in[i, k] for k in range(group))

    steps = jnp.where(side == 0, place + 1, 0)
    summed = lax.fori_loop(0, steps, one, tuple(plain[k] for k in range(group)))

    z_arrive(far0, 0)
    z_arrive(far1, 1)
    high, low = split(jnp.concatenate([far0[...], far1[...]], axis=1))
    count = slices * COLS
    y = dot(jnp.concatenate([high, low], axis=0), m_high[...])
    y = y[:count] + y[count:] + dot(high, m_low[...])
    state = jnp.zeros((COLS, NODES), F32)
    for i in range(slices):
        state = jnp.where(i <= zed, slope * state + y[i * COLS : (i + 1) * COLS], state)
    for k in range(group):
        part = slice(k * width, (k + 1) * width)
        out_ref[:, part] = summed[k] + state[:, part]

    all_of(near0, send_sems.at[0], recv0).wait_send()
    all_of(near12, send_sems.at[1], recv12).wait_send()

    @pl.loop(0, group)
    def _(to):
        @pl.when(zed != group + to)
        def _():
            part_copy(to, zed).wait_send()

        @pl.when((side == 0) & (to > place))
        def _():
            half_copy(to, place).wait_send()

        @pl.when((side == 1) & (to != place))
        def _():
            sum_copy(to, place).wait_send()

    z_sent(far0, 0)
    z_sent(far1, 1)


def shards(slices, subs, starts, inverses, retain, sources, decay, admittance, partner, delay, live, block):
    vmem, smem = pltpu.VMEM, pltpu.SMEM
    group = slices // 2
    out = pl.pallas_call(
        functools.partial(kernel, slices, subs),
        out_shape=jax.ShapeDtypeStruct((COLS, NODES), F32),
        in_specs=[pl.BlockSpec(memory_space=pltpu.HBM)] * 10,
        out_specs=pl.BlockSpec(memory_space=pltpu.VMEM),
        scratch_shapes=[
            vmem((COLS, NODES), F32), vmem((COLS, NODES), F32),
            vmem((1, NODES), F32), vmem((1, NODES), F32),
            smem((1, LINES), F32), smem((1, LINES), jnp.int32), smem((1, LINES), jnp.int32),
            smem((1, LINES), jnp.int32), smem((1, LINES), jnp.int32),
            vmem((NODES, NODES), F32), vmem((NODES, NODES), BF16), vmem((NODES, NODES), BF16),
            vmem((5, NODES // TERM, TERM, LANES), F32), vmem((4, LANES, NODES), F32),
            vmem((NODES, 2 * LANES), BF16),
            vmem((2 * LANES, NODES), BF16), vmem((2 * LANES, NODES), BF16),
            vmem((3, LINES * TERM, LANES), F32),
            vmem((subs, LINES, LANES), F32), vmem((subs, 2, LINES, LANES), F32),
            vmem((group, COLS, NODES // group), F32), vmem((slices, COLS, NODES // group), F32),
            vmem((group, group, COLS, NODES // group), F32),
            vmem((group, COLS, NODES // group), F32), vmem((group, COLS, NODES // group), F32),
            vmem((slices * COLS, LANES), F32), vmem((slices * COLS, LANES), F32),
            pltpu.SemaphoreType.DMA((9,)), pltpu.SemaphoreType.DMA((CHUNKS,)),
            pltpu.SemaphoreType.DMA((2,)), pltpu.SemaphoreType.DMA, pltpu.SemaphoreType.DMA,
            pltpu.SemaphoreType.DMA((2, slices)), pltpu.SemaphoreType.DMA((2, slices)),
            pltpu.SemaphoreType.DMA((group,)), pltpu.SemaphoreType.DMA((slices,)),
            pltpu.SemaphoreType.DMA((group,)), pltpu.SemaphoreType.DMA((group,)),
            pltpu.SemaphoreType.DMA((group,)), pltpu.SemaphoreType.DMA((group,)),
            pltpu.SemaphoreType.REGULAR((slices,)),
        ],
        compiler_params=pltpu.CompilerParams(
            collective_id=0, has_side_effects=True, vmem_limit_bytes=48 * 1024 * 1024
        ),
    )(*[pltpu.with_memory_space_constraint(a, pltpu.HBM) for a in (
        starts.reshape(COLS, NODES), inverses.reshape(NODES, NODES), retain,
        sources.reshape(COLS, NODES), decay, admittance, partner, delay, live, block,
    )])
    return out.reshape(1, 1, COLS, NODES)


def solution(mesh):
    return jax.shard_map(
        functools.partial(shards, mesh.shape["tm"], mesh.shape["sub"]),
        mesh=mesh,
        in_specs=(
            P("tm", "sub", None, None),
            P("sub", None, None),
            P("sub", None),
            P("sub", None, None),
            P("sub", None),
            P("sub", None),
            P("sub", None),
            P("sub", None),
            P("sub", None),
            P("sub", None),
        ),
        out_specs=P("tm", "sub", None, None),
        check_vma=False,
    )
```
